128 devices in a mesh: rep: 1, data: 128 (over z, y, x, core).
Axes of the slice: x: 4, y: 4, z: 4, core: 2. Of those that a mesh axis runs over, the one named last changes fastest.
Arguments:
- hidden: bfloat16 [32768, 3072], P(('rep', 'data'))
- adapter_id: int32 [32768], P(('rep', 'data'))
- w_gate: bfloat16 [3072, 8192], replicated
- w_up: bfloat16 [3072, 8192], replicated
- w_down: bfloat16 [8192, 3072], replicated
- a_gate: bfloat16 [256, 3072, 8], replicated
- b_gate: bfloat16 [256, 8, 8192], P('data')
- a_up: bfloat16 [256, 3072, 8], replicated
- b_up: bfloat16 [256, 8, 8192], P('data')
- a_down: bfloat16 [256, 8192, 8], replicated
- b_down: bfloat16 [256, 8, 3072], P('data')
Outputs:
- output: bfloat16 [32768, 3072], P(('rep', 'data'))
All inputs are finite; a program needn't handle non-finite values.
Results may differ from the reference program's by a relative error of at most 0.00618975.
Values are sent between devices in bfloat16 or wider.
A program may use at most 1 GiB of HBM per device.

```python
import jax
import jax.numpy as jnp
from jax import lax

D = 3072
FF = 8192
RANK = 8
ADAPTERS = 256
GROUP = 128
TOKENS_DEV = 256
TOKENS = 32768
CAP = 8
PER_OWNER = ADAPTERS // GROUP
ROW_BLOCK = min(64, TOKENS)
LORA_SCALE = 2.0


def draw_ids(key):
    key_hot, key_src, key_one, key_two = jax.random.split(key, 4)
    hot_owner = jax.random.randint(key_hot, (), 0, GROUP)

    def one_source(src_key):
        key_slot, key_order = jax.random.split(src_key)
        slot_order = jax.random.permutation(key_slot, (GROUP - 1) * (CAP - 1))
        extra_rank = slot_order[:TOKENS_DEV - CAP - GROUP + 1] // (CAP - 1)
        other_rank = jnp.concatenate([jnp.arange(GROUP - 1, dtype=jnp.int32), extra_rank.astype(jnp.int32)])
        other_owner = other_rank + (other_rank >= hot_owner).astype(jnp.int32)
        owner_ids = jnp.concatenate([jnp.full((CAP,), hot_owner, jnp.int32), other_owner])
        return jax.random.permutation(key_order, owner_ids)

    owner_ids = jax.vmap(one_source)(jax.random.split(key_src, GROUP)).reshape(TOKENS)
    pick_one = jax.random.randint(key_one, (TOKENS,), 0, PER_OWNER)
    pick_two = jax.random.randint(key_two, (TOKENS,), 0, PER_OWNER)
    return (owner_ids * PER_OWNER + jnp.minimum(pick_one, pick_two)).astype(jnp.int32)


def weight(key, shape, scale):
    return (jax.random.normal(key, shape, jnp.float32) * scale).astype(jnp.bfloat16)


def setup_inputs(seed: int = 0, part: int = 0) -> dict:
    base_key = jax.random.key(seed)
    part_key = jax.random.fold_in(base_key, part)
    key_rows, key_ids = jax.random.split(part_key)
    keys = jax.random.split(base_key, 9)
    return {
        'hidden': jax.random.normal(key_rows, (TOKENS, D), jnp.float32).astype(jnp.bfloat16),
        'adapter_id': draw_ids(key_ids),
        'w_gate': weight(keys[0], (D, FF), D ** -0.5),
        'w_up': weight(keys[1], (D, FF), D ** -0.5),
        'w_down': weight(keys[2], (FF, D), FF ** -0.5),
        'a_gate': weight(keys[3], (ADAPTERS, D, RANK), D ** -0.5),
        'b_gate': weight(keys[4], (ADAPTERS, RANK, FF), 0.15 * RANK ** -0.5),
        'a_up': weight(keys[5], (ADAPTERS, D, RANK), D ** -0.5),
        'b_up': weight(keys[6], (ADAPTERS, RANK, FF), 0.15 * RANK ** -0.5),
        'a_down': weight(keys[7], (ADAPTERS, FF, RANK), FF ** -0.5),
        'b_down': weight(keys[8], (ADAPTERS, RANK, D), 0.25 * RANK ** -0.5),
    }


def lora_delta(act_rows, a_rows, b_rows):
    low_rows = jnp.einsum('tk,tkr->tr', act_rows.astype(jnp.float32), a_rows.astype(jnp.float32)).astype(jnp.bfloat16)
    full_rows = jnp.einsum('tr,trm->tm', low_rows.astype(jnp.float32), b_rows.astype(jnp.float32))
    return (LORA_SCALE * full_rows).astype(jnp.bfloat16)


def reference(hidden, adapter_id, w_gate, w_up, w_down, a_gate, b_gate, a_up, b_up, a_down, b_down):
    def one_block(block):
        block_rows, block_ids = block
        gate_act = jnp.dot(block_rows, w_gate, preferred_element_type=jnp.float32) + lora_delta(block_rows, a_gate[block_ids], b_gate[block_ids]).astype(jnp.float32)
        up_act = jnp.dot(block_rows, w_up, preferred_element_type=jnp.float32) + lora_delta(block_rows, a_up[block_ids], b_up[block_ids]).astype(jnp.float32)
        hid_act = (jax.nn.silu(gate_act) * up_act).astype(jnp.bfloat16)
        down_act = jnp.dot(hid_act, w_down, preferred_element_type=jnp.float32) + lora_delta(hid_act, a_down[block_ids], b_down[block_ids]).astype(jnp.float32)
        return (block_rows.astype(jnp.float32) + down_act).astype(jnp.bfloat16)

    out_blocks = lax.map(one_block, (hidden.reshape(TOKENS // ROW_BLOCK, ROW_BLOCK, D), adapter_id.reshape(TOKENS // ROW_BLOCK, ROW_BLOCK)))
    return out_blocks.reshape(TOKENS, D)
```

```python
import jax
import jax.numpy as jnp
from jax import lax
from jax.experimental import pallas as pl
from jax.experimental.pallas import tpu as pltpu
from jax.sharding import PartitionSpec as P

SCALE = 2.0
BF = jnp.bfloat16
F32 = jnp.float32
NT = (((1,), (1,)), ((), ()))
TN = (((0,), (0,)), ((), ()))
TILE = 512
ROWS = 256


def iota(shape, dim):
    return lax.broadcasted_iota(jnp.int32, shape, dim)


def select_rows(rank):
    return jnp.where(iota((16, ROWS), 0) == (iota((16, ROWS), 1) & (rank - 1)), 1.0, 0.0).astype(BF)


def pack_low(low, ids):
    row = iota(low.shape, 0)
    return jnp.where(row < 8, low, jnp.where(row == 8, (ids & 15).astype(F32), jnp.where(row == 9, (ids >> 4).astype(F32), 0.0))).astype(BF)


def spread_low(packet, spread, tokens):
    row, col = iota((16, 384), 0), iota((16, 384), 1)
    pick = jnp.where(col < 128, jnp.where((row < 8) & (row == (col & 7)), 1.0, 0.0),
                     jnp.where(row == jnp.where(col < 256, 8, 9), 1.0, 0.0)).astype(BF)
    wide = lax.dot_general(packet, pick, TN, preferred_element_type=F32)
    lane = (iota((tokens, 128), 1) >> 3).astype(F32)
    mine = jnp.where(wide[:, 128:256] == lane, wide[:, :128], 0.0)
    block = wide[:, 256:]
    for b in range(spread.shape[1] // 128):
        spread[:, b * 128:(b + 1) * 128] = jnp.where(block == float(b), mine, 0.0).astype(BF)


def hidden_kernel(dims, x, ids, ids_up, ag, au, wg, wu, bg, bu, h,
                  wbuf, acc, bsl, snd, rec, spread, low, pk, rpk,
                  w_sem, a_sem, s0_s, s0_r, s1_s, s1_r, s2_s, s2_r, own_sem, p_s, p_r, d_s, d_r, h_sem):
    nx, ny, nz = dims
    nq = 2 * nx
    tokens, width = x.shape
    hidden = wg.shape[1]
    rows = ag.shape[0]
    slab = hidden // nq
    half = slab // 2
    tile = half
    tiles = hidden // tile
    rank = 8
    me = lax.axis_index('data')
    c, px, py, pz = me % 2, (me // 2) % nx, (me // (2 * nx)) % ny, me // (2 * nx * ny)

    def dev(z, y, xx, cc):
        return {'data': ((z * ny + y) * nx + xx) * 2 + cc}

    def at(t, l, m, z, cc):
        return dev(z, m, l, cc) if t == 0 else dev(z, l, m, cc)

    line = [px, py]
    other = [py, px]
    mine = [line[t] * 2 + c for t in range(2)]

    def member(t, q):
        return at(t, q // 2, other[t], pz, q % 2)

    barrier = pltpu.get_barrier_semaphore()
    partners = []
    for t in range(2):
        partners += [member(t, (mine[t] + k) % nq) for k in range(1, nq) if not (t == 1 and k == 0)]
    partners += [dev((pz + k) % nz, py, px, c) for k in range(1, nz)]
    for p in partners:
        pl.semaphore_signal(barrier, inc=1, device_id=p, device_id_type=pl.DeviceIdType.MESH)

    def w_copy(i, t):
        s = (i % 2) * 2 + t
        return pltpu.make_async_copy((wg, wu)[t].at[:, pl.ds(pl.multiple_of(i * tile, 128), tile)], wbuf.at[s], w_sem.at[s])

    chunks = width // tile

    def a_copies(i, t):
        s = (i % 2) * 2 + t
        return [pltpu.make_async_copy((ag, au)[t].at[pl.ds(pl.multiple_of(i * ROWS, ROWS), ROWS), pl.ds(j * tile, tile)],
                                      snd.at[s * chunks + j], a_sem.at[s, j]) for j in range(chunks)]

    for i in range(min(2, rows // ROWS)):
        for t in range(2):
            for cp in a_copies(i, t):
                cp.start()
    for i in range(2):
        for t in range(2):
            w_copy(i, t).start()

    pl.semaphore_wait(barrier, len(partners))

    bsrc = (bg, bu)

    def own(t, hf):
        col = pl.multiple_of(mine[t] * slab + hf * half, 128)
        return pltpu.make_async_copy(bsrc[t].at[:, pl.ds(col, half)],
                                     bsl.at[t, hf, pz, other[t], pl.ds(pl.multiple_of(mine[t] * 16, 16), 16)], own_sem.at[t, hf])

    def stage0(t, hf, k):
        q = (mine[t] + k) % nq
        col = pl.multiple_of(q * slab + hf * half, 128)
        return pltpu.make_async_remote_copy(
            bsrc[t].at[:, pl.ds(col, half)], bsl.at[t, hf, pz, other[t], pl.ds(pl.multiple_of(mine[t] * 16, 16), 16)],
            s0_s.at[t, hf, k], s0_r.at[t, hf, k], device_id=member(t, q), device_id_type=pl.DeviceIdType.MESH)

    def along(t, hf, k):
        if hf == 0:
            n = ny if t == 0 else nx
            return at(t, line[t], (other[t] + k) % n, pz, c)
        return at(t, line[t], other[t], (pz + k) % nz, c)

    def count(t, hf):
        return (ny if t == 0 else nx) if hf == 0 else nz

    def stage1(t, hf, k):
        ref = bsl.at[t, hf, pz, other[t]]
        return pltpu.make_async_remote_copy(ref, ref, s1_s.at[t, hf, k], s1_r.at[t, hf, k],
                                            device_id=along(t, hf, k), device_id_type=pl.DeviceIdType.MESH)

    def stage2(t, hf, k):
        ref = bsl.at[t, hf, pz] if hf == 0 else bsl.at[t, hf, :, other[t]]
        return pltpu.make_async_remote_copy(ref, ref, s2_s.at[t, hf, k], s2_r.at[t, hf, k],
                                            device_id=along(t, 1 - hf, k), device_id_type=pl.DeviceIdType.MESH)

    both = [(t, hf) for t in range(2) for hf in range(2)]
    for t, hf in both:
        own(t, hf).start()
        for k in range(1, nq):
            stage0(t, hf, k).start()

    def low_block(i, _):
        sel = select_rows(rank)
        for t in range(2):
            s = (i % 2) * 2 + t
            total = jnp.zeros((ROWS, tokens), F32)
            for j, cp in enumerate(a_copies(i, t)):
                cp.wait()
                total += lax.dot_general(snd[s * chunks + j], x[:, j * tile:(j + 1) * tile], NT, preferred_element_type=F32)
            adapter = (iota((ROWS, tokens), 0) + i * ROWS) >> 3
            kept = jnp.where(adapter == ids[...], total, 0.0).astype(BF)
            low[t] += jnp.dot(sel, kept, preferred_element_type=F32)

            @pl.when(i + 2 < rows // ROWS)
            def _():
                for cp in a_copies(i + 2, t):
                    cp.start()
        return 0

    low[...] = jnp.zeros_like(low)
    nblk = rows // ROWS
    first = max(1, nblk // 4)
    lax.fori_loop(0, first, low_block, 0)

    for t, hf in both:
        own(t, hf).wait()
        for k in range(1, nq):
            stage0(t, hf, k).wait()
    for t, hf in both:
        for k in range(1, count(t, hf)):
            stage1(t, hf, k).start()

    lax.fori_loop(first, nblk, low_block, 0)

    def packet(t, k):
        return pltpu.make_async_remote_copy(pk.at[t], rpk.at[t, k], p_s.at[t, k], p_r.at[t, k],
                                            device_id=member(t, (mine[t] + k) % nq), device_id_type=pl.DeviceIdType.MESH)

    for t in range(2):
        pk[t] = pack_low(low[t], (ids, ids_up)[t][...])
        for k in range(1, nq):
            packet(t, k).start()

    def base_tile(i, _):
        for t in range(2):
            s = (i % 2) * 2 + t
            w_copy(i, t).wait()
            acc[t, i] = jnp.dot(x[...], wbuf[s], preferred_element_type=F32)

            @pl.when(i + 2 < tiles)
            def _():
                w_copy(i + 2, t).start()
        return 0

    early = tiles // 4
    lax.fori_loop(0, early, base_tile, 0)
    for t, hf in both:
        for k in range(1, count(t, hf)):
            stage1(t, hf, k).wait()
        for k in range(1, count(t, 1 - hf)):
            stage2(t, hf, k).start()
    lax.fori_loop(early, tiles, base_tile, 0)

    for t in range(2):
        for k in range(1, nq):
            packet(t, k).wait()
    for t, hf in both:
        for k in range(1, count(t, 1 - hf)):
            stage2(t, hf, k).wait()

    def back(t, k):
        s = 2 * (t * nq + k)
        return pltpu.make_async_remote_copy(snd.at[pl.ds(s, 2)], rec.at[t, mine[t]], d_s.at[t, k], d_r.at[t, k],
                                            device_id=member(t, (mine[t] + nq - k) % nq), device_id_type=pl.DeviceIdType.MESH)

    for k in range(1, nq + 1):
        for t in range(2):
            kk = k % nq
            if kk:
                spread_low(rpk[t, kk], spread, tokens)
            else:
                spread_low(pk[t], spread, tokens)
            for hf in range(2):
                out = jnp.dot(spread[...], bsl[t, hf].reshape(rows, half), preferred_element_type=F32)
                out = (SCALE * out).astype(BF)
                if kk:
                    snd[2 * (t * nq + kk) + hf] = out
                else:
                    rec[t, mine[t], hf] = out
            if kk:
                back(t, kk).start()

    for k in range(1, nq):
        for t in range(2):
            back(t, k).wait()

    def h_copy(i):
        return pltpu.make_async_copy(rec.at[0, i // 2, i % 2], h.at[:, pl.ds(pl.multiple_of(i * tile, 128), tile)], h_sem.at[i])

    def final(i, _):
        q, hf = i // 2, i % 2
        g = acc[0, i] + rec[0, q, hf].astype(F32)
        u = acc[1, i] + rec[1, q, hf].astype(F32)
        rec[0, q, hf] = (g * jax.nn.sigmoid(g) * u).astype(BF)
        h_copy(i).start()
        return 0

    lax.fori_loop(0, tiles, final, 0)
    lax.fori_loop(0, tiles, lambda i, _: (h_copy(i).wait(), 0)[1], 0)


def hidden_call(dims, x, ids, ids_up, ag, au, wg, wu, bg, bu):
    nx, ny, nz = dims
    nq = 2 * nx
    tokens, width = x.shape
    rows, hidden = ag.shape[0], wg.shape[1]
    half = hidden // nq // 2
    tiles = hidden // half
    dma = pltpu.SemaphoreType.DMA
    vm = pl.BlockSpec(memory_space=pltpu.VMEM)
    anym = pl.BlockSpec(memory_space=pl.ANY)
    n1 = max(nx, ny, nz)
    import functools
    return pl.pallas_call(
        functools.partial(hidden_kernel, dims),
        out_shape=jax.ShapeDtypeStruct((tokens, hidden), BF),
        in_specs=[vm] * 3 + [anym] * 6,
        out_specs=anym,
        scratch_shapes=[
            pltpu.VMEM((4, width, half), BF),
            pltpu.VMEM((2, tiles, tokens, half), F32),
            pltpu.VMEM((2, 2, nz, nx, nx * 32, half), BF),
            pltpu.VMEM((4 * nq, tokens, half), BF),
            pltpu.VMEM((2, nq, 2, tokens, half), BF),
            pltpu.VMEM((tokens, rows), BF),
            pltpu.VMEM((2, 16, tokens), F32),
            pltpu.VMEM((2, 16, tokens), BF),
            pltpu.VMEM((2, nq, 16, tokens), BF),
            dma((4,)), dma((4, width // half)),
            dma((2, 2, nq)), dma((2, 2, nq)), dma((2, 2, n1)), dma((2, 2, n1)), dma((2, 2, n1)), dma((2, 2, n1)),
            dma((2, 2)), dma((2, nq)), dma((2, nq)), dma((2, nq)), dma((2, nq)), dma((tiles,)),
        ],
        compiler_params=pltpu.CompilerParams(collective_id=0, has_side_effects=True, vmem_limit_bytes=67_000_000),
        cost_estimate=pl.CostEstimate(flops=6 * tokens * width * hidden, bytes_accessed=4 * width * hidden, transcendentals=tokens * hidden),
        name='hidden',
    )(x, ids, ids_up, ag, au, wg, wu, bg, bu)


def down_kernel(x, ids, h, ad, bd, wd, out, abuf, wbuf, bbuf, spread, low, a_sem, w_sem, b_sem):
    tokens, width = x.shape
    hidden = h.shape[1]
    rows = ad.shape[0]
    nblk = rows // ROWS
    tile = min(TILE, width)
    kt = hidden // 2
    steps = width // tile

    def a_copy(i):
        return pltpu.make_async_copy(ad.at[pl.ds(pl.multiple_of(i * ROWS, ROWS), ROWS)], abuf.at[i % 3], a_sem.at[i % 3])

    def w_copy(i, k):
        s = (i % 2) * 2 + k
        return pltpu.make_async_copy(wd.at[pl.ds(k * kt, kt), pl.ds(pl.multiple_of(i * tile, 128), tile)], wbuf.at[s], w_sem.at[s])

    def b_copy(i):
        return pltpu.make_async_copy(bd.at[:, pl.ds(pl.multiple_of(i * tile, 128), tile)], bbuf.at[i % 2], b_sem.at[i % 2])

    for i in range(min(3, nblk)):
        a_copy(i).start()
    for i in range(min(2, steps)):
        b_copy(i).start()
        for k in range(2):
            w_copy(i, k).start()
    low[...] = jnp.zeros_like(low)

    def low_block(i, _):
        a_copy(i).wait()
        total = lax.dot_general(abuf[i % 3], h[...], NT, preferred_element_type=F32)
        adapter = (iota((ROWS, tokens), 0) + i * ROWS) >> 3
        kept = jnp.where(adapter == ids[...], total, 0.0).astype(BF)
        low[...] += jnp.dot(select_rows(8), kept, preferred_element_type=F32)

        @pl.when(i + 3 < nblk)
        def _():
            a_copy(i + 3).start()
        return 0

    lax.fori_loop(0, nblk, low_block, 0)
    spread_low(pack_low(low[...], ids[...]), spread, tokens)

    def step(i, _):
        b_copy(i).wait()
        delta = (SCALE * jnp.dot(spread[...], bbuf[i % 2], preferred_element_type=F32)).astype(BF).astype(F32)
        w_copy(i, 0).wait()
        y = jnp.dot(h[:, :kt], wbuf[(i % 2) * 2], preferred_element_type=F32)
        w_copy(i, 1).wait()
        y += jnp.dot(h[:, kt:], wbuf[(i % 2) * 2 + 1], preferred_element_type=F32)
        cols = pl.ds(pl.multiple_of(i * tile, 128), tile)
        out[:, cols] = (x[:, cols].astype(F32) + (y + delta)).astype(BF)

        @pl.when(i + 2 < steps)
        def _():
            b_copy(i + 2).start()
            w_copy(i + 2, 0).start()
            w_copy(i + 2, 1).start()
        return 0

    lax.fori_loop(0, steps, step, 0)


def down_call(x, ids, h, ad, bd, wd):
    tokens, width = x.shape
    rows, hidden = ad.shape
    tile = min(TILE, width)
    dma = pltpu.SemaphoreType.DMA
    vm = pl.BlockSpec(memory_space=pltpu.VMEM)
    anym = pl.BlockSpec(memory_space=pl.ANY)
    return pl.pallas_call(
        down_kernel,
        out_shape=jax.ShapeDtypeStruct((tokens, width), BF),
        in_specs=[vm] * 3 + [anym] * 3,
        out_specs=vm,
        scratch_shapes=[
            pltpu.VMEM((3, ROWS, hidden), BF),
            pltpu.VMEM((4, hidden // 2, tile), BF),
            pltpu.VMEM((2, rows, tile), BF),
            pltpu.VMEM((tokens, rows), BF),
            pltpu.VMEM((16, tokens), F32),
            dma((3,)), dma((4,)), dma((2,)),
        ],
        compiler_params=pltpu.CompilerParams(vmem_limit_bytes=67_000_000),
        cost_estimate=pl.CostEstimate(flops=2 * tokens * width * hidden, bytes_accessed=4 * width * hidden, transcendentals=0),
        name='down',
    )(x, ids, h, ad, bd, wd)


def solution(mesh, dims=(4, 4, 4)):
    row_spec = P(('rep', 'data'), None)
    tok_spec = P(('rep', 'data'))
    two = P(None, None)
    three = P(None, None, None)
    owned = P('data', None, None)
    nx, ny, nz = dims

    def device_fn(x, ids, wg, wu, wd, ag, bg, au, bu, ad, bd):
        own, r, f = bg.shape
        adapters = ag.shape[0]
        flat = lambda a: jnp.transpose(a, (0, 2, 1)).reshape(adapters * r, a.shape[1])
        b_down = lax.all_gather(bd.reshape(own * r, bd.shape[2]), 'data', axis=0, tiled=True)
        lx, ly, w = 2 * own, 2 * own * nx, nx
        rest, xs, ys = ids % lx, (ids // lx) % nx, (ids // ly) % ny
        zs = ids // (ly * ny)
        ids_up = ((zs * nx + xs) * ny + ys) * lx + rest
        ids1 = ids.reshape(1, -1)
        h = hidden_call(dims, x, ids1, ids_up.reshape(1, -1), flat(ag), flat(au), wg, wu, bg.reshape(own * r, f), bu.reshape(own * r, f))
        return down_call(x, ids1, h, flat(ad), b_down, wd)

    return jax.shard_map(device_fn, mesh=mesh, in_specs=(row_spec, tok_spec, two, two, two, three, owned, three, owned, three, owned), out_specs=row_spec, check_vma=False)
```

```python
import functools

import jax
import jax.numpy as jnp
from jax import lax
from jax.experimental import pallas as pl
from jax.experimental.pallas import tpu as pltpu
from jax.sharding import PartitionSpec as P

SCALE = 2.0
BF = jnp.bfloat16
F32 = jnp.float32
NT = (((1,), (1,)), ((), ()))
TN = (((0,), (0,)), ((), ()))
TILE = 512
ROWS = 256


def iota(shape, dim):
    return lax.broadcasted_iota(jnp.int32, shape, dim)


def select_rows(rank):
    return jnp.where(iota((16, ROWS), 0) == (iota((16, ROWS), 1) & (rank - 1)), 1.0, 0.0).astype(BF)


def pack_low(low, ids):
    row = iota(low.shape, 0)
    return jnp.where(row < 8, low, jnp.where(row == 8, (ids & 15).astype(F32), jnp.where(row == 9, (ids >> 4).astype(F32), 0.0))).astype(BF)


def spread_low(packet, spread, tokens):
    row, col = iota((16, 384), 0), iota((16, 384), 1)
    pick = jnp.where(col < 128, jnp.where((row < 8) & (row == (col & 7)), 1.0, 0.0),
                     jnp.where(row == jnp.where(col < 256, 8, 9), 1.0, 0.0)).astype(BF)
    wide = lax.dot_general(packet, pick, TN, preferred_element_type=F32)
    lane = (iota((tokens, 128), 1) >> 3).astype(F32)
    mine = jnp.where(wide[:, 128:256] == lane, wide[:, :128], 0.0)
    block = wide[:, 256:]
    for b in range(spread.shape[1] // 128):
        spread[:, b * 128:(b + 1) * 128] = jnp.where(block == float(b), mine, 0.0).astype(BF)


def hidden_kernel(dims, x, ids, ids_up, ag, au, wg, wu, bg, bu, ad, wd, y, pkd,
                  wbuf, acc, b0, b1, snd, rec, spread, low, adn, pk, rpk,
                  w_sem, a_sem, s0_s, s0_r, s1_s, s1_r, s2_s, s2_r, own_sem, p_s, p_r, d_s, d_r):
    nx, ny, nz = dims
    nq = 2 * nx
    tokens, width = x.shape
    hidden = wg.shape[1]
    rows = ag.shape[0]
    slab = hidden // nq
    tile = slab // 2
    tiles = hidden // tile
    cut = b0.shape[-1]
    bsl = (b0, b1)
    spans = (pl.ds(0, cut), pl.ds(cut, slab - cut))
    me = lax.axis_index('data')
    c, px, py, pz = me % 2, (me // 2) % nx, (me // (2 * nx)) % ny, me // (2 * nx * ny)
    mesh_id = pl.DeviceIdType.MESH

    def dev(z, yy, xx, cc):
        return {'data': ((z * ny + yy) * nx + xx) * 2 + cc}

    def at(t, l, m, z, cc):
        return dev(z, m, l, cc) if t == 0 else dev(z, l, m, cc)

    line = [px, py]
    other = [py, px]
    mine = [line[t] * 2 + c for t in range(2)]

    def member(t, q):
        return at(t, q // 2, other[t], pz, q % 2)

    barrier = pltpu.get_barrier_semaphore()
    partners = []
    for t in range(2):
        partners += [member(t, (mine[t] + k) % nq) for k in range(1, nq)]
    partners += [dev((pz + k) % nz, py, px, c) for k in range(1, nz)]
    for p in partners:
        pl.semaphore_signal(barrier, inc=1, device_id=p, device_id_type=mesh_id)

    chunks = width // tile

    def w_copies(i, t):
        s = (i % 2) * 2 + t
        cols = pl.ds(pl.multiple_of(i * tile, 128), tile)
        return [pltpu.make_async_copy((wg, wu)[t].at[pl.ds(j * tile, tile), cols], wbuf.at[s, j], w_sem.at[s, j]) for j in range(chunks)]

    def tile_at(n):
        return 2 * ((2 * (px + py) + c + n // 2) % nq) + n % 2

    def d_copies(n, t):
        s = (n % 2) * 2 + t
        i = tile_at(n)
        span = pl.ds(pl.multiple_of(i * tile, 128), tile)
        if t == 0:
            return [pltpu.make_async_copy(ad.at[pl.ds(j * tile, tile), span], wbuf.at[s, j], w_sem.at[s, j]) for j in range(rows // tile)]
        return [pltpu.make_async_copy(wd.at[span, pl.ds(j * tile, tile)], wbuf.at[s, j], w_sem.at[s, j]) for j in range(chunks)]

    wide = width // slab

    def a_copies(i, t):
        s = (i % 2) * 2 + t
        return [pltpu.make_async_copy((ag, au)[t].at[pl.ds(pl.multiple_of(i * ROWS, ROWS), ROWS), pl.ds(j * slab, slab)],
                                      snd.at[s * wide + j], a_sem.at[s, j]) for j in range(wide)]

    def start(copies):
        for cp in copies:
            cp.start()

    def wait(copies):
        for cp in copies:
            cp.wait()

    for i in range(min(2, rows // ROWS)):
        for t in range(2):
            start(a_copies(i, t))
    for i in range(2):
        for t in range(2):
            start(w_copies(i, t))

    pl.semaphore_wait(barrier, len(partners))

    bsrc = (bg, bu)
    widths = (cut, slab - cut)

    def own_rows(t, hf):
        return bsl[hf].at[t, pz, other[t], pl.ds(pl.multiple_of(mine[t] * 16, 16), 16)]

    def source(t, hf, q):
        return bsrc[t].at[:, pl.ds(pl.multiple_of(q * slab + hf * cut, 128), widths[hf])]

    def own(t, hf):
        return pltpu.make_async_copy(source(t, hf, mine[t]), own_rows(t, hf), own_sem.at[t, hf])

    def stage0(t, hf, k):
        q = (mine[t] + k) % nq
        return pltpu.make_async_remote_copy(source(t, hf, q), own_rows(t, hf), s0_s.at[t, hf, k], s0_r.at[t, hf, k],
                                            device_id=member(t, q), device_id_type=mesh_id)

    def count(t, hf):
        return (ny if t == 0 else nx) if hf == 0 else nz

    def along(t, hf, k):
        if hf == 0:
            return at(t, line[t], (other[t] + k) % count(t, 0), pz, c)
        return at(t, line[t], other[t], (pz + k) % nz, c)

    def block(t, hf, b):
        if hf == 0:
            return bsl[0].at[t, pz, (other[t] + b) % count(t, 0)]
        return bsl[1].at[t, (pz + b) % nz, other[t]]

    def stage1(t, hf, k):
        ref = block(t, hf, 0)
        return pltpu.make_async_remote_copy(ref, ref, s1_s.at[t, hf, k], s1_r.at[t, hf, k],
                                            device_id=along(t, hf, k), device_id_type=mesh_id)

    def stage2(t, hf, k, b):
        ref = block(t, hf, b)
        return pltpu.make_async_remote_copy(ref, ref, s2_s.at[t, hf, k, b], s2_r.at[t, hf, k, b],
                                            device_id=along(t, 1 - hf, k), device_id_type=mesh_id)

    both = [(t, hf) for hf in (1, 0) for t in range(2)]
    for t, hf in both:
        own(t, hf).start()
        for k in range(1, nq):
            stage0(t, hf, k).start()

    nblk = rows // ROWS

    def low_block(i, _):
        sel = select_rows(8)
        for t in range(2):
            s = (i % 2) * 2 + t
            total = jnp.zeros((ROWS, tokens), F32)
            for j, cp in enumerate(a_copies(i, t)):
                cp.wait()
                total += lax.dot_general(snd[s * wide + j], x[:, j * slab:(j + 1) * slab], NT, preferred_element_type=F32)
            adapter = (iota((ROWS, tokens), 0) + i * ROWS) >> 3
            kept = jnp.where(adapter == ids[...], total, 0.0).astype(BF)
            low[t] += jnp.dot(sel, kept, preferred_element_type=F32)

            @pl.when(i + 2 < nblk)
            def _():
                start(a_copies(i + 2, t))
        return 0

    low[...] = jnp.zeros_like(low)
    first = max(1, nblk // 4)
    lax.fori_loop(0, first, low_block, 0)

    for t, hf in both:
        own(t, hf).wait()
        wait([stage0(t, hf, k) for k in range(1, nq)])
        start([stage1(t, hf, k) for k in range(1, count(t, hf))])
    for t, hf in both:
        start([stage2(t, hf, k, 0) for k in range(1, count(t, 1 - hf))])

    lax.fori_loop(first, nblk, low_block, 0)

    def packet(t, k):
        return pltpu.make_async_remote_copy(pk.at[t], rpk.at[t, mine[t]], p_s.at[t, k], p_r.at[t, k],
                                            device_id=member(t, (mine[t] + k) % nq), device_id_type=mesh_id)

    for t in range(2):
        pk[t] = pack_low(low[t], (ids, ids_up)[t][...])
        rpk[t, mine[t]] = pk[t]
        for k in range(1, nq):
            packet(t, k).start()

    def relay(t, hf):
        n = count(t, hf)
        for k in range(1, n):
            stage1(t, hf, k).wait()
            start([stage2(t, hf, kk, n - k) for kk in range(1, count(t, 1 - hf))])

    for t in range(2):
        relay(t, 0)

    def base_tile(i, _):
        for t in range(2):
            s = (i % 2) * 2 + t
            wait(w_copies(i, t))
            acc[t, i] = jnp.dot(x[...], wbuf[s, :chunks].reshape(width, tile), preferred_element_type=F32)

            @pl.when(i + 2 < tiles)
            def _():
                start(w_copies(i + 2, t))

            @pl.when(i + 2 >= tiles)
            def _():
                start(d_copies(i + 2 - tiles, t))
        return 0

    early = tiles // 8
    lax.fori_loop(0, early, base_tile, 0)
    for t in range(2):
        relay(t, 1)
    lax.fori_loop(early, tiles, base_tile, 0)

    for t in range(2):
        for k in range(1, nq):
            packet(t, k).wait()
    for t, hf in both:
        for k in range(1, count(t, 1 - hf)):
            for b in range(count(t, hf)):
                stage2(t, hf, k, b).wait()

    def back(t, k, d):
        return pltpu.make_async_remote_copy(snd.at[t * nq + k], rec.at[t, mine[t]], d_s.at[t, k], d_r.at[t, k],
                                            device_id=member(t, d), device_id_type=mesh_id)

    def target(t, k):
        return (mine[t] + 4 * nq - 2 * other[t] - k) % nq

    def delta_step(k, _):
        for t in range(2):
            d = target(t, k)
            spread_low(rpk[t, d], spread, tokens)
            for hf in range(2):
                out = jnp.dot(spread[...], bsl[hf][t].reshape(rows, widths[hf]), preferred_element_type=F32)
                snd[t * nq + k, :, spans[hf]] = (SCALE * out).astype(BF)

            @pl.when(d == mine[t])
            def _():
                rec[t, mine[t]] = snd[t * nq + k]

            @pl.when(d != mine[t])
            def _():
                back(t, k, d).start()
        return 0

    lax.fori_loop(0, nq, delta_step, 0)

    y[...] = jnp.zeros_like(y)
    adn[...] = jnp.zeros_like(adn)

    def final(k, _):
        q = (2 * (px + py) + c + k) % nq
        for t in range(2):
            @pl.when(q != mine[t])
            def _():
                pltpu.make_async_remote_copy(snd.at[t * nq + k], rec.at[t, q], d_s.at[t, k], d_r.at[t, k],
                                             device_id=member(t, target(t, k)), device_id_type=mesh_id).wait_recv()
        for hf in range(2):
            n = 2 * k + hf
            cols = pl.ds(hf * tile, tile)
            g = acc[0, 2 * q + hf] + rec[0, q, :, cols].astype(F32)
            u = acc[1, 2 * q + hf] + rec[1, q, :, cols].astype(F32)
            h = (g * jax.nn.sigmoid(g) * u).astype(BF)
            wait(d_copies(n, 0))
            for j in range(rows // tile):
                span = pl.ds(j * tile, tile)
                adn[span] += lax.dot_general(wbuf[2 * hf, j], h, NT, preferred_element_type=F32)
            wait(d_copies(n, 1))
            for j in range(chunks):
                span = pl.ds(j * tile, tile)
                y[:, span] += jnp.dot(h, wbuf[2 * hf + 1, j], preferred_element_type=F32)

            @pl.when(n + 2 < tiles)
            def _():
                for t in range(2):
                    start(d_copies(n + 2, t))
        return 0

    lax.fori_loop(0, nq, final, 0)

    low[0] = jnp.zeros_like(low[0])

    def down_block(i, _):
        adapter = (iota((ROWS, tokens), 0) + i * ROWS) >> 3
        kept = jnp.where(adapter == ids[...], adn[pl.ds(pl.multiple_of(i * ROWS, ROWS), ROWS)], 0.0).astype(BF)
        low[0] += jnp.dot(select_rows(8), kept, preferred_element_type=F32)
        return 0

    lax.fori_loop(0, nblk, down_block, 0)
    pkd[...] = pack_low(low[0], ids[...])

    def sent(k, _):
        for t in range(2):
            d = target(t, k)

            @pl.when(d != mine[t])
            def _():
                back(t, k, d).wait_send()
        return 0

    lax.fori_loop(0, nq, sent, 0)


def hidden_call(dims, x, ids, ids_up, ag, au, wg, wu, bg, bu, ad, wd):
    nx, ny, nz = dims
    nq = 2 * nx
    tokens, width = x.shape
    rows, hidden = ag.shape[0], wg.shape[1]
    slab = hidden // nq
    tile = slab // 2
    cut = max(128, slab // 4)
    tiles = hidden // tile
    dma = pltpu.SemaphoreType.DMA
    vm = pl.BlockSpec(memory_space=pltpu.VMEM)
    anym = pl.BlockSpec(memory_space=pl.ANY)
    n1 = max(nx, ny, nz)
    nch = max(width, rows) // tile
    return pl.pallas_call(
        functools.partial(hidden_kernel, dims),
        out_shape=[jax.ShapeDtypeStruct((tokens, width), F32), jax.ShapeDtypeStruct((16, tokens), BF)],
        in_specs=[vm] * 3 + [anym] * 8,
        out_specs=[vm, vm],
        scratch_shapes=[
            pltpu.VMEM((4, nch, tile, tile), BF),
            pltpu.VMEM((2, tiles, tokens, tile), F32),
            pltpu.VMEM((2, nz, nx, nx * 32, cut), BF),
            pltpu.VMEM((2, nz, nx, nx * 32, slab - cut), BF),
            pltpu.VMEM((2 * nq, tokens, slab), BF),
            pltpu.VMEM((2, nq, tokens, slab), BF),
            pltpu.VMEM((tokens, rows), BF),
            pltpu.VMEM((2, 16, tokens), F32),
            pltpu.VMEM((rows, tokens), F32),
            pltpu.VMEM((2, 16, tokens), BF),
            pltpu.VMEM((2, nq, 16, tokens), BF),
            dma((4, nch)), dma((4, width // slab)),
            dma((2, 2, nq)), dma((2, 2, nq)), dma((2, 2, n1)), dma((2, 2, n1)), dma((2, 2, n1, n1)), dma((2, 2, n1, n1)),
            dma((2, 2)), dma((2, nq)), dma((2, nq)), dma((2, nq)), dma((2, nq)),
        ],
        compiler_params=pltpu.CompilerParams(collective_id=0, has_side_effects=True, vmem_limit_bytes=67_000_000),
        cost_estimate=pl.CostEstimate(flops=6 * tokens * width * hidden, bytes_accessed=6 * width * hidden, transcendentals=tokens * hidden),
        name='hidden',
    )(x, ids, ids_up, ag, au, wg, wu, bg, bu, ad, wd)


def down_kernel(x, y, packet, bd, out, spread):
    @pl.when(pl.program_id(0) == 0)
    def _():
        spread_low(packet[...], spread, x.shape[0])

    delta = (SCALE * jnp.dot(spread[...], bd[...], preferred_element_type=F32)).astype(BF).astype(F32)
    out[...] = (x[...].astype(F32) + (y[...] + delta)).astype(BF)


def down_call(x, y, packet, bd):
    tokens, width = x.shape
    rows = bd.shape[0]
    tile = min(TILE, width)
    rowblk = pl.BlockSpec((tokens, tile), lambda i: (0, i))
    return pl.pallas_call(
        down_kernel,
        grid=(width // tile,),
        out_shape=jax.ShapeDtypeStruct((tokens, width), BF),
        in_specs=[rowblk, rowblk, pl.BlockSpec((16, tokens), lambda i: (0, 0)), pl.BlockSpec((rows, tile), lambda i: (0, i))],
        out_specs=rowblk,
        scratch_shapes=[pltpu.VMEM((tokens, rows), BF)],
        cost_estimate=pl.CostEstimate(flops=2 * tokens * width * rows, bytes_accessed=2 * width * rows, transcendentals=0),
        name='down',
    )(x, y, packet, bd)


def solution(mesh, dims=(4, 4, 4)):
    row_spec = P(('rep', 'data'), None)
    tok_spec = P(('rep', 'data'))
    two = P(None, None)
    three = P(None, None, None)
    owned = P('data', None, None)
    nx, ny, nz = dims

    def device_fn(x, ids, wg, wu, wd, ag, bg, au, bu, ad, bd):
        own, r, f = bg.shape
        adapters = ag.shape[0]
        flat = lambda a: jnp.transpose(a, (0, 2, 1)).reshape(adapters * r, a.shape[1])
        b_down = lax.all_gather(bd.reshape(own * r, bd.shape[2]), 'data', axis=0, tiled=True)
        lx, ly = 2 * own, 2 * own * nx
        rest, xs, ys = ids % lx, (ids // lx) % nx, (ids // ly) % ny
        zs = ids // (ly * ny)
        ids_up = ((zs * nx + xs) * ny + ys) * lx + rest
        ids1 = ids.reshape(1, -1)
        y, packet = hidden_call(dims, x, ids1, ids_up.reshape(1, -1), flat(ag), flat(au), wg, wu, bg.reshape(own * r, f), bu.reshape(own * r, f), flat(ad), wd)
        return down_call(x, y, packet, b_down)

    return jax.shard_map(device_fn, mesh=mesh, in_specs=(row_spec, tok_spec, two, two, two, three, owned, three, owned, three, owned), out_specs=row_spec, check_vma=False)
```

```python
import functools

import jax
import jax.numpy as jnp
from jax import lax
from jax.experimental import pallas as pl
from jax.experimental.pallas import tpu as pltpu
from jax.sharding import PartitionSpec as P

SCALE = 2.0
BF = jnp.bfloat16
F32 = jnp.float32
NT = (((1,), (1,)), ((), ()))
TN = (((0,), (0,)), ((), ()))
ROWS = 256


def iota(shape, dim):
    return lax.broadcasted_iota(jnp.int32, shape, dim)


def select_rows(rank):
    return jnp.where(iota((16, ROWS), 0) == (iota((16, ROWS), 1) & (rank - 1)), 1.0, 0.0).astype(BF)


def pack_low(low, ids):
    row = iota(low.shape, 0)
    return jnp.where(row < 8, low, jnp.where(row == 8, (ids & 15).astype(F32), jnp.where(row == 9, (ids >> 4).astype(F32), 0.0))).astype(BF)


def spread_low(packet, spread, tokens):
    row, col = iota((16, 384), 0), iota((16, 384), 1)
    pick = jnp.where(col < 128, jnp.where((row < 8) & (row == (col & 7)), 1.0, 0.0),
                     jnp.where(row == jnp.where(col < 256, 8, 9), 1.0, 0.0)).astype(BF)
    wide = lax.dot_general(packet, pick, TN, preferred_element_type=F32)
    lane = (iota((tokens, 128), 1) >> 3).astype(F32)
    mine = jnp.where(wide[:, 128:256] == lane, wide[:, :128], 0.0)
    block = wide[:, 256:]
    for b in range(spread.shape[1] // 128):
        spread[:, b * 128:(b + 1) * 128] = jnp.where(block == float(b), mine, 0.0).astype(BF)


def layer_kernel(dims, x, ids, ag, au, wg, wu, bg, bu, ad, wd, bd, out,
                 wbuf, acc, b0, b1, b2, b3, snd, rec, spread, low, adn, y, pk, rpk,
                  w_sem, a_sem, s0_s, s0_r, s1_s, s1_r, s2_s, s2_r, own_sem, p_s, p_r, d_s, d_r, o_sem):
    bits = [n.bit_length() - 1 for n in (2 * (bg.shape[0] // 8), dims[0], dims[1])]
    low_mask, xs = ids[...] & ((1 << bits[0]) - 1), (ids[...] >> bits[0]) & (dims[0] - 1)
    ys, zs = (ids[...] >> (bits[0] + bits[1])) & (dims[1] - 1), ids[...] >> sum(bits)
    ids_up = (((zs * dims[0] + xs) * dims[1] + ys) << bits[0]) + low_mask
    nx, ny, nz = dims
    nq = 2 * nx
    tokens, width = x.shape
    hidden = wg.shape[1]
    rows = ag.shape[0]
    slab = hidden // nq
    tile = slab // 2
    tiles = hidden // tile
    cut = b0.shape[-1]
    spans = (pl.ds(0, cut), pl.ds(cut, slab - cut))
    me = lax.axis_index('data')
    c, px, py, pz = me % 2, (me // 2) % nx, (me // (2 * nx)) % ny, me // (2 * nx * ny)
    mesh_id = pl.DeviceIdType.MESH

    def dev(z, yy, xx, cc):
        return {'data': ((z * ny + yy) * nx + xx) * 2 + cc}

    def at(t, l, m, z, cc):
        return dev(z, m, l, cc) if t % 2 == 0 else dev(z, l, m, cc)

    line = [px, py, px, py]
    other = [py, px, py, px]
    mine = [line[t] * 2 + c for t in range(4)]

    def member(t, q):
        return at(t, q // 2, other[t], pz, q % 2)

    barrier = pltpu.get_barrier_semaphore()
    partners = []
    for t in range(2):
        partners += [member(t, (mine[t] + k) % nq) for k in range(1, nq)]
    partners += [dev((pz + k) % nz, py, px, c) for k in range(1, nz)]
    for p in partners:
        pl.semaphore_signal(barrier, inc=1, device_id=p, device_id_type=mesh_id)

    chunks = width // tile

    def w_copies(i, t):
        s = (i % 2) * 2 + t
        cols = pl.ds(pl.multiple_of(i * tile, 128), tile)
        return [pltpu.make_async_copy((wg, wu)[t].at[pl.ds(j * tile, tile), cols], wbuf.at[s, j], w_sem.at[s, j]) for j in range(chunks)]

    def tile_at(n):
        return 2 * ((2 * (px + py) + c + n // 2) % nq) + n % 2

    def d_copies(n, t):
        s = (n % 2) * 2 + t
        i = tile_at(n)
        span = pl.ds(pl.multiple_of(i * tile, 128), tile)
        if t == 0:
            return [pltpu.make_async_copy(ad.at[pl.ds(j * tile, tile), span], wbuf.at[s, j], w_sem.at[s, j]) for j in range(rows // tile)]
        return [pltpu.make_async_copy(wd.at[span, pl.ds(j * tile, tile)], wbuf.at[s, j], w_sem.at[s, j]) for j in range(chunks)]

    wide = width // slab

    def a_copies(i, t):
        s = (i % 2) * 2 + t
        return [pltpu.make_async_copy((ag, au)[t].at[pl.ds(pl.multiple_of(i * ROWS, ROWS), ROWS), pl.ds(j * slab, slab)],
                                      snd.at[s * wide + j], a_sem.at[s, j]) for j in range(wide)]

    def start(copies):
        for cp in copies:
            cp.start()

    def wait(copies):
        for cp in copies:
            cp.wait()

    for i in range(min(2, rows // ROWS)):
        for t in range(2):
            start(a_copies(i, t))
    for i in range(2):
        for t in range(2):
            start(w_copies(i, t))

    pl.semaphore_wait(barrier, len(partners))

    w2, w3 = b2.shape[-1], b3.shape[-1]
    slots = {(0, 0): 0, (0, 1): 1, (1, 0): 2, (1, 1): 3, (2, 0): 4, (3, 0): 5}
    widths = (cut, slab - cut)

    def held(t, hf):
        return (b0, b1)[hf].at[t] if t < 2 else (b2, b3)[t - 2]

    def own_rows(t, hf):
        return held(t, hf).at[pz, other[t], pl.ds(pl.multiple_of(mine[t] * 16, 16), 16)]

    def source(t, hf, q):
        if t < 2:
            return (bg, bu)[t].at[:, pl.ds(pl.multiple_of(q * slab + hf * cut, 128), widths[hf])]
        return bd.at[:, pl.ds(pl.multiple_of(q * w2 if t == 2 else nq * w2 + q * w3, 128), w2 if t == 2 else w3)]

    def own(t, hf):
        return pltpu.make_async_copy(source(t, hf, mine[t]), own_rows(t, hf), own_sem.at[slots[t, hf]])

    def stage0(t, hf, k):
        q, g = (mine[t] + k) % nq, slots[t, hf]
        return pltpu.make_async_remote_copy(source(t, hf, q), own_rows(t, hf), s0_s.at[g, k], s0_r.at[g, k],
                                            device_id=member(t, q), device_id_type=mesh_id)

    def count(t, hf):
        return (ny if t % 2 == 0 else nx) if hf == 0 else nz

    def along(t, hf, k):
        if hf == 0:
            return at(t, line[t], (other[t] + k) % count(t, 0), pz, c)
        return at(t, line[t], other[t], (pz + k) % nz, c)

    def block(t, hf, b):
        if hf == 0:
            return held(t, hf).at[pz, (other[t] + b) % count(t, 0)]
        return held(t, hf).at[(pz + b) % nz, other[t]]

    def stage1(t, hf, k):
        ref = block(t, hf, 0)
        return pltpu.make_async_remote_copy(ref, ref, s1_s.at[slots[t, hf], k], s1_r.at[slots[t, hf], k],
                                            device_id=along(t, hf, k), device_id_type=mesh_id)

    def stage2(t, hf, k, b):
        ref = block(t, hf, b)
        return pltpu.make_async_remote_copy(ref, ref, s2_s.at[slots[t, hf], k, b], s2_r.at[slots[t, hf], k, b],
                                            device_id=along(t, 1 - hf, k), device_id_type=mesh_id)

    both = [(t, hf) for hf in (1, 0) for t in range(2)]
    downs = [(2, 0), (3, 0)]
    for t, hf in both + downs:
        own(t, hf).start()
        for k in range(1, nq):
            stage0(t, hf, k).start()

    nblk = rows // ROWS

    def low_block(i, _):
        sel = select_rows(8)
        for t in range(2):
            s = (i % 2) * 2 + t
            total = jnp.zeros((ROWS, tokens), F32)
            for j, cp in enumerate(a_copies(i, t)):
                cp.wait()
                total += lax.dot_general(snd[s * wide + j], x[:, j * slab:(j + 1) * slab], NT, preferred_element_type=F32)
            adapter = (iota((ROWS, tokens), 0) + i * ROWS) >> 3
            kept = jnp.where(adapter == ids[...], total, 0.0).astype(BF)
            low[t] += jnp.dot(sel, kept, preferred_element_type=F32)

            @pl.when(i + 2 < nblk)
            def _():
                start(a_copies(i + 2, t))
        return 0

    low[...] = jnp.zeros_like(low)
    first = max(1, nblk // 4)
    lax.fori_loop(0, first, low_block, 0)

    for t, hf in both:
        own(t, hf).wait()
        wait([stage0(t, hf, k) for k in range(1, nq)])
        start([stage1(t, hf, k) for k in range(1, count(t, hf))])
    for t, hf in both:
        start([stage2(t, hf, k, 0) for k in range(1, count(t, 1 - hf))])

    lax.fori_loop(first, nblk, low_block, 0)
    for t, hf in downs:
        own(t, hf).wait()
        wait([stage0(t, hf, k) for k in range(1, nq)])
        start([stage1(t, hf, k) for k in range(1, count(t, hf))])

    def packet(t, k):
        return pltpu.make_async_remote_copy(pk.at[t], rpk.at[t, mine[t]], p_s.at[t, k], p_r.at[t, k],
                                            device_id=member(t, (mine[t] + k) % nq), device_id_type=mesh_id)

    def send_packet(t, rows_in):
        pk[t] = pack_low(rows_in, ids[...] if t % 2 == 0 else ids_up)
        rpk[t, mine[t]] = pk[t]
        for k in range(1, nq):
            packet(t, k).start()

    for t in range(2):
        send_packet(t, low[t])

    def relay(t, hf):
        n = count(t, hf)
        for k in range(1, n):
            stage1(t, hf, k).wait()
            start([stage2(t, hf, kk, n - k) for kk in range(1, count(t, 1 - hf))])

    for t in range(2):
        relay(t, 0)

    def base_tile(i, _):
        for t in range(2):
            s = (i % 2) * 2 + t
            wait(w_copies(i, t))
            acc[t, i] = jnp.dot(x[...], wbuf[s, :chunks].reshape(width, tile), preferred_element_type=F32)

            @pl.when(i + 2 < tiles)
            def _():
                start(w_copies(i + 2, t))

            @pl.when(i + 2 >= tiles)
            def _():
                start(d_copies(i + 2 - tiles, t))
        return 0

    early = tiles // 8
    lax.fori_loop(0, early, base_tile, 0)
    for t in range(2):
        relay(t, 1)
    lax.fori_loop(early, tiles, base_tile, 0)
    for t, hf in downs:
        for k in range(1, count(t, hf)):
            stage1(t, hf, k).wait()
        for b in range(count(t, hf)):
            start([stage2(t, hf, k, b) for k in range(1, nz)])

    for t in range(2):
        for k in range(1, nq):
            packet(t, k).wait()
    for t, hf in both:
        for k in range(1, count(t, 1 - hf)):
            for b in range(count(t, hf)):
                stage2(t, hf, k, b).wait()

    def back(t, k, d):
        return pltpu.make_async_remote_copy(snd.at[t * nq + k], rec.at[t, mine[t]], d_s.at[t, k], d_r.at[t, k],
                                            device_id=member(t, d), device_id_type=mesh_id)

    def target(t, k):
        return (mine[t] + 4 * nq - 2 * other[t] - k) % nq

    def delta_step(k, _):
        for t in range(2):
            d = target(t, k)
            spread_low(rpk[t, d], spread, tokens)
            for hf in range(2):
                out = jnp.dot(spread[...], (b0, b1)[hf][t].reshape(rows, widths[hf]), preferred_element_type=F32)
                snd[t * nq + k, :, spans[hf]] = (SCALE * out).astype(BF)

            @pl.when(d == mine[t])
            def _():
                rec[t, mine[t]] = snd[t * nq + k]

            @pl.when(d != mine[t])
            def _():
                back(t, k, d).start()
        return 0

    lax.fori_loop(0, nq, delta_step, 0)

    y[...] = jnp.zeros_like(y)
    adn[...] = jnp.zeros_like(adn)

    def final(k, _):
        q = (2 * (px + py) + c + k) % nq
        for t in range(2):
            @pl.when(q != mine[t])
            def _():
                pltpu.make_async_remote_copy(snd.at[t * nq + k], rec.at[t, q], d_s.at[t, k], d_r.at[t, k],
                                             device_id=member(t, target(t, k)), device_id_type=mesh_id).wait_recv()
        for hf in range(2):
            n = 2 * k + hf
            cols = pl.ds(hf * tile, tile)
            g = acc[0, 2 * q + hf] + rec[0, q, :, cols].astype(F32)
            u = acc[1, 2 * q + hf] + rec[1, q, :, cols].astype(F32)
            h = (g * jax.nn.sigmoid(g) * u).astype(BF)
            wait(d_copies(n, 0))
            for j in range(rows // tile):
                span = pl.ds(j * tile, tile)
                adn[span] += lax.dot_general(wbuf[2 * hf, j], h, NT, preferred_element_type=F32)
            wait(d_copies(n, 1))
            for j in range(chunks):
                span = pl.ds(j * tile, tile)
                y[:, span] += jnp.dot(h, wbuf[2 * hf + 1, j], preferred_element_type=F32)

            @pl.when(n + 2 < tiles)
            def _():
                for t in range(2):
                    start(d_copies(n + 2, t))
        return 0

    lax.fori_loop(0, nq, final, 0)

    low[0] = jnp.zeros_like(low[0])

    def down_block(i, _):
        adapter = (iota((ROWS, tokens), 0) + i * ROWS) >> 3
        kept = jnp.where(adapter == ids[...], adn[pl.ds(pl.multiple_of(i * ROWS, ROWS), ROWS)], 0.0).astype(BF)
        low[0] += jnp.dot(select_rows(8), kept, preferred_element_type=F32)
        return 0

    lax.fori_loop(0, nblk, down_block, 0)
    for t in (2, 3):
        send_packet(t, low[0])

    def sent(k, _):
        for t in range(2):
            d = target(t, k)

            @pl.when(d != mine[t])
            def _():
                back(t, k, d).wait_send()
        return 0

    lax.fori_loop(0, nq, sent, 0)
    for t, hf in downs:
        for k in range(1, nz):
            for b in range(count(t, hf)):
                stage2(t, hf, k, b).wait()
        for k in range(1, nq):
            packet(t, k).wait()

    def down_back(t, k, q, d):
        w = pl.ds(0, w2 if t == 2 else w3)
        return pltpu.make_async_remote_copy(snd.at[(t - 2) * nq + k, :, w], rec.at[t - 2, q, :, w], d_s.at[t, k], d_r.at[t, k],
                                            device_id=member(t, d), device_id_type=mesh_id)

    def down_step(k, _):
        for t in (2, 3):
            d = target(t, k)
            w = pl.ds(0, w2 if t == 2 else w3)
            spread_low(rpk[t, d], spread, tokens)
            delta = jnp.dot(spread[...], held(t, 0)[...].reshape(rows, w2 if t == 2 else w3), preferred_element_type=F32)
            delta = (SCALE * delta).astype(BF)
            snd[(t - 2) * nq + k, :, w] = delta

            @pl.when(d == mine[t])
            def _():
                rec[t - 2, mine[t], :, w] = snd[(t - 2) * nq + k, :, w]

            @pl.when(d != mine[t])
            def _():
                down_back(t, k, mine[t], d).start()
        return 0

    lax.fori_loop(0, nq, down_step, 0)

    def out_copy(t, q):
        w = w2 if t == 2 else w3
        cols = pl.ds(pl.multiple_of(q * w2 if t == 2 else nq * w2 + q * w3, 128), w)
        return pltpu.make_async_copy(rec.at[t - 2, q, :, pl.ds(0, w)], out.at[:, cols], o_sem.at[t - 2, q])

    def finish(k, _):
        q = (2 * (px + py) + c + k) % nq
        for t in (2, 3):
            @pl.when(q != mine[t])
            def _():
                down_back(t, k, q, target(t, k)).wait_recv()
            w = w2 if t == 2 else w3
            cols = pl.ds(pl.multiple_of(q * w2 if t == 2 else nq * w2 + q * w3, 128), w)
            part = pl.ds(0, w)
            rec[t - 2, q, :, part] = (x[:, cols].astype(F32) + (y[:, cols] + rec[t - 2, q, :, part].astype(F32))).astype(BF)
            out_copy(t, q).start()
        return 0

    lax.fori_loop(0, nq, finish, 0)

    def down_sent(k, _):
        for t in (2, 3):
            d = target(t, k)

            @pl.when(d != mine[t])
            def _():
                down_back(t, k, mine[t], d).wait_send()

            out_copy(t, k).wait()
        return 0

    lax.fori_loop(0, nq, down_sent, 0)


def layer_call(dims, x, ids, ag, au, wg, wu, bg, bu, ad, wd, bd):
    nx, ny, nz = dims
    nq = 2 * nx
    tokens, width = x.shape
    rows, hidden = ag.shape[0], wg.shape[1]
    slab = hidden // nq
    tile = slab // 2
    cut = max(128, slab // 4)
    w2 = width // (3 * nq) * 2
    w3 = width // (3 * nq)
    tiles = hidden // tile
    dma = pltpu.SemaphoreType.DMA
    vm = pl.BlockSpec(memory_space=pltpu.VMEM)
    anym = pl.BlockSpec(memory_space=pl.ANY)
    n1 = max(nx, ny, nz)
    nch = max(width, rows) // tile
    wide = width // slab
    return pl.pallas_call(
        functools.partial(layer_kernel, dims),
        out_shape=jax.ShapeDtypeStruct((tokens, width), BF),
        in_specs=[vm] * 2 + [anym] * 9,
        out_specs=anym,
        scratch_shapes=[
            pltpu.VMEM((4, nch, tile, tile), BF),
            pltpu.VMEM((2, tiles, tokens, tile), F32),
            pltpu.VMEM((2, nz, nx, nx * 32, cut), BF),
            pltpu.VMEM((2, nz, nx, nx * 32, slab - cut), BF),
            pltpu.VMEM((nz, nx, nx * 32, w2), BF),
            pltpu.VMEM((nz, nx, nx * 32, w3), BF),
            pltpu.VMEM((max(2 * nq, 4 * wide), tokens, slab), BF),
            pltpu.VMEM((2, nq, tokens, slab), BF),
            pltpu.VMEM((tokens, rows), BF),
            pltpu.VMEM((2, 16, tokens), F32),
            pltpu.VMEM((rows, tokens), F32),
            pltpu.VMEM((tokens, width), F32),
            pltpu.VMEM((4, 16, tokens), BF),
            pltpu.VMEM((4, nq, 16, tokens), BF),
            dma((4, nch)), dma((4, wide)),
            dma((6, nq)), dma((6, nq)), dma((6, n1)), dma((6, n1)), dma((6, n1, n1)), dma((6, n1, n1)),
            dma((6,)), dma((4, nq)), dma((4, nq)), dma((4, nq)), dma((4, nq)), dma((2, nq)),
        ],
        compiler_params=pltpu.CompilerParams(collective_id=0, has_side_effects=True, vmem_limit_bytes=67_000_000),
        cost_estimate=pl.CostEstimate(flops=6 * tokens * width * hidden, bytes_accessed=6 * width * hidden, transcendentals=tokens * hidden),
        name='layer',
    )(x, ids, ag, au, wg, wu, bg, bu, ad, wd, bd)


def solution(mesh, dims=(4, 4, 4)):
    row_spec = P(('rep', 'data'), None)
    tok_spec = P(('rep', 'data'))
    two = P(None, None)
    three = P(None, None, None)
    owned = P('data', None, None)

    def device_fn(x, ids, wg, wu, wd, ag, bg, au, bu, ad, bd):
        own, r = bg.shape[:2]
        adapters = ag.shape[0]
        flat = lambda a: jnp.transpose(a, (0, 2, 1)).reshape(adapters * r, a.shape[1])
        rows = lambda a: a.reshape(own * r, a.shape[2])
        return layer_call(dims, x, ids.reshape(1, -1), flat(ag), flat(au), wg, wu, rows(bg), rows(bu), flat(ad), wd, rows(bd))

    return jax.shard_map(device_fn, mesh=mesh, in_specs=(row_spec, tok_spec, two, two, two, three, owned, three, owned, three, owned), out_specs=row_spec, check_vma=False)
```

```python
import functools

import jax
import jax.numpy as jnp
from jax import lax
from jax.experimental import pallas as pl
from jax.experimental.pallas import tpu as pltpu
from jax.sharding import PartitionSpec as P

SCALE = 2.0
BF = jnp.bfloat16
F32 = jnp.float32
TN = (((0,), (0,)), ((), ()))
ROWS = 256


def iota(shape, dim):
    return lax.broadcasted_iota(jnp.int32, shape, dim)


def select_rows(rank):
    return jnp.where(iota((16, ROWS), 0) == (iota((16, ROWS), 1) & (rank - 1)), 1.0, 0.0).astype(BF)


def pack_low(low, ids):
    row = iota(low.shape, 0)
    return jnp.where(row < 8, low, jnp.where(row == 8, (ids & 15).astype(F32), jnp.where(row == 9, (ids >> 4).astype(F32), 0.0))).astype(BF)


def spread_low(packet, spread, tokens):
    row, col = iota((16, 384), 0), iota((16, 384), 1)
    pick = jnp.where(col < 128, jnp.where((row < 8) & (row == (col & 7)), 1.0, 0.0),
                     jnp.where(row == jnp.where(col < 256, 8, 9), 1.0, 0.0)).astype(BF)
    wide = lax.dot_general(packet, pick, TN, preferred_element_type=F32)
    lane = (iota((tokens, 128), 1) >> 3).astype(F32)
    mine = jnp.where(wide[:, 128:256] == lane, wide[:, :128], 0.0)
    block = wide[:, 256:]
    for b in range(spread.shape[1] // 128):
        spread[:, b * 128:(b + 1) * 128] = jnp.where(block == float(b), mine, 0.0).astype(BF)


def layer_kernel(dims, x, ids, ag, au, wg, wu, bg, bu, ad, wd, bd, out,
                 wbuf, acc, b0, b1, b2, b3, snd, rec, spread, low, adn, y, pk, rpk,
                  w_sem, a_sem, s0_s, s0_r, s1_s, s1_r, s2_s, s2_r, own_sem, p_s, p_r, d_s, d_r, o_sem):
    bits = [n.bit_length() - 1 for n in (2 * (bg.shape[0] // 8), dims[0], dims[1])]
    low_mask, xs = ids[...] & ((1 << bits[0]) - 1), (ids[...] >> bits[0]) & (dims[0] - 1)
    ys, zs = (ids[...] >> (bits[0] + bits[1])) & (dims[1] - 1), ids[...] >> sum(bits)
    ids_up = (((zs * dims[0] + xs) * dims[1] + ys) << bits[0]) + low_mask
    nx, ny, nz = dims
    nq = 2 * nx
    tokens, width = x.shape
    hidden = wg.shape[1]
    rows = ag.shape[0]
    slab = hidden // nq
    tile = slab // 2
    tiles = hidden // tile
    cut = b0.shape[-1]
    spans = (pl.ds(0, cut), pl.ds(cut, slab - cut))
    me = lax.axis_index('data')
    c, px, py, pz = me % 2, (me // 2) % nx, (me // (2 * nx)) % ny, me // (2 * nx * ny)
    mesh_id = pl.DeviceIdType.MESH

    def dev(z, yy, xx, cc):
        return {'data': ((z * ny + yy) * nx + xx) * 2 + cc}

    def at(t, l, m, z, cc):
        return dev(z, m, l, cc) if t % 2 == 0 else dev(z, l, m, cc)

    line = [px, py, px, py]
    other = [py, px, py, px]
    mine = [line[t] * 2 + c for t in range(4)]

    def member(t, q):
        return at(t, q // 2, other[t], pz, q % 2)

    barrier = pltpu.get_barrier_semaphore()
    partners = []
    for t in range(2):
        partners += [member(t, (mine[t] + k) % nq) for k in range(1, nq)]
    partners += [dev((pz + k) % nz, py, px, c) for k in range(1, nz)]
    for p in partners:
        pl.semaphore_signal(barrier, inc=1, device_id=p, device_id_type=mesh_id)

    chunks = width // tile

    def w_copies(i, t):
        s = (i % 2) * 2 + t
        cols = pl.ds(pl.multiple_of(i * tile, 128), tile)
        return [pltpu.make_async_copy((wg, wu)[t].at[pl.ds(j * tile, tile), cols], wbuf.at[s, j], w_sem.at[s, j]) for j in range(chunks)]

    def tile_at(n):
        return 2 * ((2 * (px + py) + c + n // 2) % nq) + n % 2

    def d_copies(n, t):
        s = (n % 2) * 2 + t
        i = tile_at(n)
        span = pl.ds(pl.multiple_of(i * tile, 128), tile)
        if t == 0:
            return [pltpu.make_async_copy(ad.at[pl.ds(j * tile, tile), span], wbuf.at[s, j], w_sem.at[s, j]) for j in range(rows // tile)]
        return [pltpu.make_async_copy(wd.at[span, pl.ds(j * tile, tile)], wbuf.at[s, j], w_sem.at[s, j]) for j in range(chunks)]

    wide = width // slab

    def a_copies(i, t):
        s = (i % 2) * 2 + t
        return [pltpu.make_async_copy((ag, au)[t].at[pl.ds(pl.multiple_of(i * ROWS, ROWS), ROWS), pl.ds(j * slab, slab)],
                                      snd.at[s * wide + j], a_sem.at[s, j]) for j in range(wide)]

    def start(copies):
        for cp in copies:
            cp.start()

    def wait(copies):
        for cp in copies:
            cp.wait()

    for i in range(min(2, rows // ROWS)):
        for t in range(2):
            start(a_copies(i, t))
    for i in range(2):
        for t in range(2):
            start(w_copies(i, t))

    pl.semaphore_wait(barrier, len(partners))

    w2, w3 = b2.shape[-1], b3.shape[-1]
    slots = {(0, 0): 0, (0, 1): 1, (1, 0): 2, (1, 1): 3, (2, 0): 4, (3, 0): 5}
    widths = (cut, slab - cut)

    def held(t, hf):
        return (b0, b1)[hf].at[t] if t < 2 else (b2, b3)[t - 2]

    def own_rows(t, hf):
        return held(t, hf).at[pz, other[t], pl.ds(pl.multiple_of(mine[t] * 16, 16), 16)]

    def source(t, hf, q):
        if t < 2:
            return (bg, bu)[t].at[:, pl.ds(pl.multiple_of(q * slab + hf * cut, 128), widths[hf])]
        return bd.at[:, pl.ds(pl.multiple_of(q * w2 if t == 2 else nq * w2 + q * w3, 128), w2 if t == 2 else w3)]

    def own(t, hf):
        return pltpu.make_async_copy(source(t, hf, mine[t]), own_rows(t, hf), own_sem.at[slots[t, hf]])

    def stage0(t, hf, k):
        q, g = (mine[t] + k) % nq, slots[t, hf]
        return pltpu.make_async_remote_copy(source(t, hf, q), own_rows(t, hf), s0_s.at[g, k], s0_r.at[g, k],
                                            device_id=member(t, q), device_id_type=mesh_id)

    def count(t, hf):
        return (ny if t % 2 == 0 else nx) if hf == 0 else nz

    def along(t, hf, k):
        if hf == 0:
            return at(t, line[t], (other[t] + k) % count(t, 0), pz, c)
        return at(t, line[t], other[t], (pz + k) % nz, c)

    def block(t, hf, b):
        if hf == 0:
            return held(t, hf).at[pz, (other[t] + b) % count(t, 0)]
        return held(t, hf).at[(pz + b) % nz, other[t]]

    def stage1(t, hf, k):
        ref = block(t, hf, 0)
        return pltpu.make_async_remote_copy(ref, ref, s1_s.at[slots[t, hf], k], s1_r.at[slots[t, hf], k],
                                            device_id=along(t, hf, k), device_id_type=mesh_id)

    def stage2(t, hf, k, b):
        ref = block(t, hf, b)
        return pltpu.make_async_remote_copy(ref, ref, s2_s.at[slots[t, hf], k, b], s2_r.at[slots[t, hf], k, b],
                                            device_id=along(t, 1 - hf, k), device_id_type=mesh_id)

    both = [(t, hf) for hf in (1, 0) for t in range(2)]
    downs = [(2, 0), (3, 0)]
    for t, hf in both + downs:
        own(t, hf).start()
        for k in range(1, nq):
            stage0(t, hf, k).start()

    nblk = rows // ROWS
    per = slab // tokens

    def x_turned(j):
        return snd.at[4 * wide + j // per, :, pl.ds(j % per * tokens, tokens)]

    for j in range(width // tokens):
        x_turned(j)[...] = x[:, j * tokens:(j + 1) * tokens].T

    def low_block(i, _):
        sel = select_rows(8)
        for t in range(2):
            s = (i % 2) * 2 + t
            wait(a_copies(i, t))
            total = jnp.zeros((ROWS, tokens), F32)
            for j in range(width // tokens):
                total += jnp.dot(snd[s * wide + j // per, :, pl.ds(j % per * tokens, tokens)], x_turned(j)[...], preferred_element_type=F32)
            adapter = (iota((ROWS, tokens), 0) + i * ROWS) >> 3
            kept = jnp.where(adapter == ids[...], total, 0.0).astype(BF)
            low[t] += jnp.dot(sel, kept, preferred_element_type=F32)

            @pl.when(i + 2 < nblk)
            def _():
                start(a_copies(i + 2, t))
        return 0

    low[...] = jnp.zeros_like(low)
    first = max(1, nblk // 4)
    lax.fori_loop(0, first, low_block, 0)

    for t, hf in both:
        own(t, hf).wait()
        wait([stage0(t, hf, k) for k in range(1, nq)])
        start([stage1(t, hf, k) for k in range(1, count(t, hf))])
    for t, hf in both:
        start([stage2(t, hf, k, 0) for k in range(1, count(t, 1 - hf))])

    lax.fori_loop(first, nblk, low_block, 0)
    for t, hf in downs:
        own(t, hf).wait()
        wait([stage0(t, hf, k) for k in range(1, nq)])
        start([stage1(t, hf, k) for k in range(1, count(t, hf))])

    def packet(t, k):
        return pltpu.make_async_remote_copy(pk.at[t], rpk.at[t, mine[t]], p_s.at[t, k], p_r.at[t, k],
                                            device_id=member(t, (mine[t] + k) % nq), device_id_type=mesh_id)

    def send_packet(t, rows_in):
        pk[t] = pack_low(rows_in, ids[...] if t % 2 == 0 else ids_up)
        rpk[t, mine[t]] = pk[t]
        for k in range(1, nq):
            packet(t, k).start()

    for t in range(2):
        send_packet(t, low[t])

    def relay(t, hf):
        n = count(t, hf)
        for k in range(1, n):
            stage1(t, hf, k).wait()
            start([stage2(t, hf, kk, n - k) for kk in range(1, count(t, 1 - hf))])

    for t in range(2):
        relay(t, 0)

    def base_tile(i, _):
        for t in range(2):
            s = (i % 2) * 2 + t
            wait(w_copies(i, t))
            acc[t, i] = jnp.dot(x[...], wbuf[s, :chunks].reshape(width, tile), preferred_element_type=F32)

            @pl.when(i + 2 < tiles)
            def _():
                start(w_copies(i + 2, t))

            @pl.when(i + 2 >= tiles)
            def _():
                start(d_copies(i + 2 - tiles, t))
        return 0

    early = tiles // 8
    lax.fori_loop(0, early, base_tile, 0)
    for t in range(2):
        relay(t, 1)
    lax.fori_loop(early, tiles, base_tile, 0)
    for t, hf in downs:
        for k in range(1, count(t, hf)):
            stage1(t, hf, k).wait()
        for b in range(count(t, hf)):
            start([stage2(t, hf, k, b) for k in range(1, nz)])

    for t in range(2):
        for k in range(1, nq):
            packet(t, k).wait()
    for t, hf in both:
        for k in range(1, count(t, 1 - hf)):
            for b in range(count(t, hf)):
                stage2(t, hf, k, b).wait()

    def back(t, k, d):
        return pltpu.make_async_remote_copy(snd.at[t * nq + k], rec.at[t, mine[t]], d_s.at[t, k], d_r.at[t, k],
                                            device_id=member(t, d), device_id_type=mesh_id)

    def target(t, k):
        return (mine[t] + 4 * nq - 2 * other[t] - k) % nq

    def delta_step(k):
        aims = [target(t, k) for t in range(2)]
        for t in range(2):
            spread_low(rpk[t, aims[t]], spread.at[t], tokens)
            for hf in range(2):
                out_part = jnp.dot(spread[t], (b0, b1)[hf][t].reshape(rows, widths[hf]), preferred_element_type=F32)
                snd[t * nq + k, :, spans[hf]] = (SCALE * out_part).astype(BF)
        for t in range(2):
            @pl.when(aims[t] == mine[t])
            def _():
                rec[t, mine[t]] = snd[t * nq + k]

            @pl.when(aims[t] != mine[t])
            def _():
                back(t, k, aims[t]).start()

    def final(k):
        q = (2 * (px + py) + c + k) % nq
        for t in range(2):
            @pl.when(q != mine[t])
            def _():
                pltpu.make_async_remote_copy(snd.at[t * nq + k], rec.at[t, q], d_s.at[t, k], d_r.at[t, k],
                                             device_id=member(t, target(t, k)), device_id_type=mesh_id).wait_recv()

        def gated(hf):
            cols = pl.ds(hf * tile, tile)
            g = acc[0, 2 * q + hf] + rec[0, q, :, cols].astype(F32)
            u = acc[1, 2 * q + hf] + rec[1, q, :, cols].astype(F32)
            rec[0, q, :, cols] = (g * jax.nn.sigmoid(g) * u).astype(BF)

        for hf in range(2):
            n = 2 * k + hf
            wait(d_copies(n, 0))
            wait(d_copies(n, 1))
            if hf == 0:
                gated(0)
            h = rec[0, q, :, pl.ds(hf * tile, tile)]
            turned = h.T
            for j in range(rows // tile):
                span = pl.ds(j * tile, tile)
                adn[span] += jnp.dot(wbuf[2 * hf, j], turned, preferred_element_type=F32)
            for j in range(chunks):
                span = pl.ds(j * tile, tile)
                y[:, span] += jnp.dot(h, wbuf[2 * hf + 1, j], preferred_element_type=F32)
            if hf == 0:
                gated(1)

            @pl.when(n + 2 < tiles)
            def _():
                for t in range(2):
                    start(d_copies(n + 2, t))

    y[...] = jnp.zeros_like(y)
    adn[...] = jnp.zeros_like(adn)
    lag = nq

    def middle(k, _):
        @pl.when(k < nq)
        def _():
            delta_step(k)

        @pl.when(k >= lag)
        def _():
            final(k - lag)
        return 0

    lax.fori_loop(0, nq + lag, middle, 0)

    low[0] = jnp.zeros_like(low[0])

    def down_block(i, _):
        adapter = (iota((ROWS, tokens), 0) + i * ROWS) >> 3
        kept = jnp.where(adapter == ids[...], adn[pl.ds(pl.multiple_of(i * ROWS, ROWS), ROWS)], 0.0).astype(BF)
        low[0] += jnp.dot(select_rows(8), kept, preferred_element_type=F32)
        return 0

    lax.fori_loop(0, nblk, down_block, 0)
    for t in (2, 3):
        send_packet(t, low[0])

    def sent(k, _):
        for t in range(2):
            d = target(t, k)

            @pl.when(d != mine[t])
            def _():
                back(t, k, d).wait_send()
        return 0

    lax.fori_loop(0, nq, sent, 0)
    for t, hf in downs:
        for k in range(1, nz):
            for b in range(count(t, hf)):
                stage2(t, hf, k, b).wait()
        for k in range(1, nq):
            packet(t, k).wait()

    def down_back(t, k, q, d):
        w = pl.ds(0, w2 if t == 2 else w3)
        return pltpu.make_async_remote_copy(snd.at[(t - 2) * nq + k, :, w], rec.at[t - 2, q, :, w], d_s.at[t, k], d_r.at[t, k],
                                            device_id=member(t, d), device_id_type=mesh_id)

    def down_step(k, _):
        aims = [target(t, k) for t in (2, 3)]
        parts = [pl.ds(0, w2), pl.ds(0, w3)]
        for i in range(2):
            spread_low(rpk[i + 2, aims[i]], spread.at[i], tokens)
            delta = jnp.dot(spread[i], (b2, b3)[i][...].reshape(rows, (w2, w3)[i]), preferred_element_type=F32)
            snd[i * nq + k, :, parts[i]] = (SCALE * delta).astype(BF)
        for i in range(2):
            @pl.when(aims[i] == mine[i + 2])
            def _():
                rec[i, mine[i + 2], :, parts[i]] = snd[i * nq + k, :, parts[i]]

            @pl.when(aims[i] != mine[i + 2])
            def _():
                down_back(i + 2, k, mine[i + 2], aims[i]).start()
        return 0

    lax.fori_loop(0, nq, down_step, 0)

    def out_copy(t, q):
        w = w2 if t == 2 else w3
        cols = pl.ds(pl.multiple_of(q * w2 if t == 2 else nq * w2 + q * w3, 128), w)
        return pltpu.make_async_copy(rec.at[t - 2, q, :, pl.ds(0, w)], out.at[:, cols], o_sem.at[t - 2, q])

    def finish(k, _):
        q = (2 * (px + py) + c + k) % nq
        for t in (2, 3):
            @pl.when(q != mine[t])
            def _():
                down_back(t, k, q, target(t, k)).wait_recv()
            w = w2 if t == 2 else w3
            cols = pl.ds(pl.multiple_of(q * w2 if t == 2 else nq * w2 + q * w3, 128), w)
            part = pl.ds(0, w)
            rec[t - 2, q, :, part] = (x[:, cols].astype(F32) + (y[:, cols] + rec[t - 2, q, :, part].astype(F32))).astype(BF)
            out_copy(t, q).start()
        return 0

    lax.fori_loop(0, nq, finish, 0)

    def down_sent(k, _):
        for t in (2, 3):
            d = target(t, k)

            @pl.when(d != mine[t])
            def _():
                down_back(t, k, mine[t], d).wait_send()

            out_copy(t, k).wait()
        return 0

    lax.fori_loop(0, nq, down_sent, 0)


def layer_call(dims, x, ids, ag, au, wg, wu, bg, bu, ad, wd, bd):
    nx, ny, nz = dims
    nq = 2 * nx
    tokens, width = x.shape
    rows, hidden = ag.shape[0], wg.shape[1]
    slab = hidden // nq
    tile = slab // 2
    cut = max(128, slab // 4)
    w2 = width // (3 * nq) * 2
    w3 = width // (3 * nq)
    tiles = hidden // tile
    dma = pltpu.SemaphoreType.DMA
    vm = pl.BlockSpec(memory_space=pltpu.VMEM)
    anym = pl.BlockSpec(memory_space=pl.ANY)
    n1 = max(nx, ny, nz)
    nch = max(width, rows) // tile
    wide = width // slab
    return pl.pallas_call(
        functools.partial(layer_kernel, dims),
        out_shape=jax.ShapeDtypeStruct((tokens, width), BF),
        in_specs=[vm] * 2 + [anym] * 9,
        out_specs=anym,
        scratch_shapes=[
            pltpu.VMEM((4, nch, tile, tile), BF),
            pltpu.VMEM((2, tiles, tokens, tile), F32),
            pltpu.VMEM((2, nz, nx, nx * 32, cut), BF),
            pltpu.VMEM((2, nz, nx, nx * 32, slab - cut), BF),
            pltpu.VMEM((nz, nx, nx * 32, w2), BF),
            pltpu.VMEM((nz, nx, nx * 32, w3), BF),
            pltpu.VMEM((max(2 * nq, 5 * wide), tokens, slab), BF),
            pltpu.VMEM((2, nq, tokens, slab), BF),
            pltpu.VMEM((2, tokens, rows), BF),
            pltpu.VMEM((2, 16, tokens), F32),
            pltpu.VMEM((rows, tokens), F32),
            pltpu.VMEM((tokens, width), F32),
            pltpu.VMEM((4, 16, tokens), BF),
            pltpu.VMEM((4, nq, 16, tokens), BF),
            dma((4, nch)), dma((4, wide)),
            dma((6, nq)), dma((6, nq)), dma((6, n1)), dma((6, n1)), dma((6, n1, n1)), dma((6, n1, n1)),
            dma((6,)), dma((4, nq)), dma((4, nq)), dma((4, nq)), dma((4, nq)), dma((2, nq)),
        ],
        compiler_params=pltpu.CompilerParams(collective_id=0, has_side_effects=True, vmem_limit_bytes=67_000_000),
        cost_estimate=pl.CostEstimate(flops=6 * tokens * width * hidden, bytes_accessed=6 * width * hidden, transcendentals=tokens * hidden),
        name='layer',
    )(x, ids, ag, au, wg, wu, bg, bu, ad, wd, bd)


def solution(mesh, dims=(4, 4, 4)):
    row_spec = P(('rep', 'data'), None)
    tok_spec = P(('rep', 'data'))
    two = P(None, None)
    three = P(None, None, None)
    owned = P('data', None, None)

    def device_fn(x, ids, wg, wu, wd, ag, bg, au, bu, ad, bd):
        own, r = bg.shape[:2]
        adapters = ag.shape[0]
        flat = lambda a: jnp.transpose(a, (0, 2, 1)).reshape(adapters * r, a.shape[1])
        rows = lambda a: a.reshape(own * r, a.shape[2])
        return layer_call(dims, x, ids.reshape(1, -1), flat(ag), flat(au), wg, wu, rows(bg), rows(bu), flat(ad), wd, rows(bd))

    return jax.shard_map(device_fn, mesh=mesh, in_specs=(row_spec, tok_spec, two, two, two, three, owned, three, owned, three, owned), out_specs=row_spec, check_vma=False)
```

```python
import functools

import jax
import jax.numpy as jnp
from jax import lax
from jax.experimental import pallas as pl
from jax.experimental.pallas import tpu as pltpu
from jax.sharding import PartitionSpec as P

SCALE = 2.0
BF = jnp.bfloat16
F32 = jnp.float32
TN = (((0,), (0,)), ((), ()))
ROWS = 256


def iota(shape, dim):
    return lax.broadcasted_iota(jnp.int32, shape, dim)


def select_rows(rank):
    return jnp.where(iota((16, ROWS), 0) == (iota((16, ROWS), 1) & (rank - 1)), 1.0, 0.0).astype(BF)


def pack_low(low, ids):
    row = iota(low.shape, 0)
    return jnp.where(row < 8, low, jnp.where(row == 8, (ids & 15).astype(F32), jnp.where(row == 9, (ids >> 4).astype(F32), 0.0))).astype(BF)


def spread_low(packet, spread, tokens):
    row, col = iota((16, 384), 0), iota((16, 384), 1)
    pick = jnp.where(col < 128, jnp.where((row < 8) & (row == (col & 7)), 1.0, 0.0),
                     jnp.where(row == jnp.where(col < 256, 8, 9), 1.0, 0.0)).astype(BF)
    wide = lax.dot_general(packet, pick, TN, preferred_element_type=F32)
    lane = (iota((tokens, 128), 1) >> 3).astype(F32)
    mine = jnp.where(wide[:, 128:256] == lane, wide[:, :128], 0.0)
    block = wide[:, 256:]
    for b in range(spread.shape[1] // 128):
        spread[:, b * 128:(b + 1) * 128] = jnp.where(block == float(b), mine, 0.0).astype(BF)


def layer_kernel(dims, x, ids, ag, au, wg, wu, bg, bu, ad, wd, bd, out,
                 wbuf, acc, b0, b1, b2, b3, snd, rec, spread, low, adn, y, pk, rpk,
                  w_sem, a_sem, s0_s, s0_r, s1_s, s1_r, s2_s, s2_r, own_sem, p_s, p_r, d_s, d_r, o_sem):
    bits = [n.bit_length() - 1 for n in (2 * (bg.shape[0] // 8), dims[0], dims[1])]
    low_mask, xs = ids[...] & ((1 << bits[0]) - 1), (ids[...] >> bits[0]) & (dims[0] - 1)
    ys, zs = (ids[...] >> (bits[0] + bits[1])) & (dims[1] - 1), ids[...] >> sum(bits)
    ids_up = (((zs * dims[0] + xs) * dims[1] + ys) << bits[0]) + low_mask
    nx, ny, nz = dims
    nq = 2 * nx
    tokens, width = x.shape
    hidden = wg.shape[1]
    rows = ag.shape[0]
    slab = hidden // nq
    tile = slab // 2
    tiles = hidden // tile
    cut = b0.shape[-1]
    spans = (pl.ds(0, cut), pl.ds(cut, slab - cut))
    me = lax.axis_index('data')
    c, px, py, pz = me % 2, (me // 2) % nx, (me // (2 * nx)) % ny, me // (2 * nx * ny)
    mesh_id = pl.DeviceIdType.MESH

    def dev(z, yy, xx, cc):
        return {'data': ((z * ny + yy) * nx + xx) * 2 + cc}

    def at(t, l, m, z, cc):
        return dev(z, m, l, cc) if t % 2 == 0 else dev(z, l, m, cc)

    line = [px, py, px, py]
    other = [py, px, py, px]
    mine = [line[t] * 2 + c for t in range(4)]

    def member(t, q):
        return at(t, q // 2, other[t], pz, q % 2)

    barrier = pltpu.get_barrier_semaphore()
    partners = []
    for t in range(2):
        partners += [member(t, (mine[t] + k) % nq) for k in range(1, nq)]
    partners += [dev((pz + k) % nz, py, px, c) for k in range(1, nz)]
    for p in partners:
        pl.semaphore_signal(barrier, inc=1, device_id=p, device_id_type=mesh_id)

    chunks = width // tile

    def w_copies(i, t):
        s = (i % 2) * 2 + t
        cols = pl.ds(pl.multiple_of(i * tile, 128), tile)
        return [pltpu.make_async_copy((wg, wu)[t].at[pl.ds(j * tile, tile), cols], wbuf.at[s, j], w_sem.at[s, j]) for j in range(chunks)]

    def slab_at(k):
        i = k % nx
        hop = 3 * ((i + 1) // 2) - i if nx == 4 else i
        return (px + hop) % nx * 2 + (c + k // nx) % 2

    def tile_at(n):
        return 2 * slab_at(n // 2) + n % 2

    def target(t, k):
        far = nx - 1
        last = k // (2 * far)
        r = k % far
        hop = (1 - last) * (2 - r + 3 * (r // 2) if nx == 4 else 1)
        flip = (1 - last) * (k // far) + last * (nq - 1 - k)
        return (line[t] + nx - hop) % nx * 2 + (c + flip) % 2

    def d_copies(n, t):
        s = (n % 2) * 2 + t
        i = tile_at(n)
        span = pl.ds(pl.multiple_of(i * tile, 128), tile)
        if t == 0:
            return [pltpu.make_async_copy(ad.at[pl.ds(j * tile, tile), span], wbuf.at[s, j], w_sem.at[s, j]) for j in range(rows // tile)]
        return [pltpu.make_async_copy(wd.at[span, pl.ds(j * tile, tile)], wbuf.at[s, j], w_sem.at[s, j]) for j in range(chunks)]

    wide = width // slab

    def a_copies(i, t):
        s = (i % 2) * 2 + t
        return [pltpu.make_async_copy((ag, au)[t].at[pl.ds(pl.multiple_of(i * ROWS, ROWS), ROWS), pl.ds(j * slab, slab)],
                                      snd.at[s * wide + j], a_sem.at[s, j]) for j in range(wide)]

    def order(n):
        return [2, 1, 3] if n == 4 else list(range(1, n))

    def start(copies):
        for cp in copies:
            cp.start()

    def wait(copies):
        for cp in copies:
            cp.wait()

    for i in range(min(2, rows // ROWS)):
        for t in range(2):
            start(a_copies(i, t))
    for i in range(2):
        for t in range(2):
            start(w_copies(i, t))

    pl.semaphore_wait(barrier, len(partners))

    w2, w3 = b2.shape[-1], b3.shape[-1]
    slots = {(0, 0): 0, (0, 1): 1, (1, 0): 2, (1, 1): 3, (2, 0): 4, (3, 0): 5}
    widths = (cut, slab - cut)

    def held(t, hf):
        return (b0, b1)[hf].at[t] if t < 2 else (b2, b3)[t - 2]

    def own_rows(t, hf):
        return held(t, hf).at[pz, other[t], pl.ds(pl.multiple_of(mine[t] * 16, 16), 16)]

    def source(t, hf, q):
        if t < 2:
            return (bg, bu)[t].at[:, pl.ds(pl.multiple_of(q * slab + hf * cut, 128), widths[hf])]
        return bd.at[:, pl.ds(pl.multiple_of(q * w2 if t == 2 else nq * w2 + q * w3, 128), w2 if t == 2 else w3)]

    def own(t, hf):
        return pltpu.make_async_copy(source(t, hf, mine[t]), own_rows(t, hf), own_sem.at[slots[t, hf]])

    def stage0(t, hf, k):
        q, g = (mine[t] + k) % nq, slots[t, hf]
        return pltpu.make_async_remote_copy(source(t, hf, q), own_rows(t, hf), s0_s.at[g, k], s0_r.at[g, k],
                                            device_id=member(t, q), device_id_type=mesh_id)

    def count(t, hf):
        return (ny if t % 2 == 0 else nx) if hf == 0 else nz

    def along(t, hf, k):
        if hf == 0:
            return at(t, line[t], (other[t] + k) % count(t, 0), pz, c)
        return at(t, line[t], other[t], (pz + k) % nz, c)

    def block(t, hf, b):
        if hf == 0:
            return held(t, hf).at[pz, (other[t] + b) % count(t, 0)]
        return held(t, hf).at[(pz + b) % nz, other[t]]

    def stage1(t, hf, k):
        ref = block(t, hf, 0)
        return pltpu.make_async_remote_copy(ref, ref, s1_s.at[slots[t, hf], k], s1_r.at[slots[t, hf], k],
                                            device_id=along(t, hf, k), device_id_type=mesh_id)

    def stage2(t, hf, k, b):
        ref = block(t, hf, b)
        return pltpu.make_async_remote_copy(ref, ref, s2_s.at[slots[t, hf], k, b], s2_r.at[slots[t, hf], k, b],
                                            device_id=along(t, 1 - hf, k), device_id_type=mesh_id)

    both = [(t, hf) for hf in (1, 0) for t in range(2)]
    downs = [(2, 0), (3, 0)]
    for t, hf in both + downs:
        own(t, hf).start()
        for k in range(1, nq):
            stage0(t, hf, k).start()

    nblk = rows // ROWS
    per = slab // tokens

    def x_turned(j):
        return snd.at[4 * wide + j // per, :, pl.ds(j % per * tokens, tokens)]

    for j in range(width // tokens):
        x_turned(j)[...] = x[:, j * tokens:(j + 1) * tokens].T

    def low_block(i, _):
        sel = select_rows(8)
        for t in range(2):
            s = (i % 2) * 2 + t
            wait(a_copies(i, t))
            total = jnp.zeros((ROWS, tokens), F32)
            for j in range(width // tokens):
                total += jnp.dot(snd[s * wide + j // per, :, pl.ds(j % per * tokens, tokens)], x_turned(j)[...], preferred_element_type=F32)
            adapter = (iota((ROWS, tokens), 0) + i * ROWS) >> 3
            kept = jnp.where(adapter == ids[...], total, 0.0).astype(BF)
            low[t] += jnp.dot(sel, kept, preferred_element_type=F32)

            @pl.when(i + 2 < nblk)
            def _():
                start(a_copies(i + 2, t))
        return 0

    low[...] = jnp.zeros_like(low)
    first = max(1, nblk // 4)
    lax.fori_loop(0, first, low_block, 0)

    for t, hf in both:
        own(t, hf).wait()
        wait([stage0(t, hf, k) for k in range(1, nq)])
        start([stage1(t, hf, k) for k in order(count(t, hf))])
    for t, hf in both:
        start([stage2(t, hf, k, 0) for k in order(count(t, 1 - hf))])

    lax.fori_loop(first, nblk, low_block, 0)
    for t, hf in downs:
        own(t, hf).wait()
        wait([stage0(t, hf, k) for k in range(1, nq)])
        start([stage1(t, hf, k) for k in order(count(t, hf))])

    def packet(t, k):
        return pltpu.make_async_remote_copy(pk.at[t], rpk.at[t, mine[t]], p_s.at[t, k], p_r.at[t, k],
                                            device_id=member(t, (mine[t] + k) % nq), device_id_type=mesh_id)

    def send_packet(t, rows_in):
        pk[t] = pack_low(rows_in, ids[...] if t % 2 == 0 else ids_up)
        rpk[t, mine[t]] = pk[t]
        for k in range(1, nq):
            packet(t, k).start()

    for t in range(2):
        send_packet(t, low[t])

    def relay(t, hf):
        n = count(t, hf)
        for k in range(1, n):
            stage1(t, hf, k).wait()
            start([stage2(t, hf, kk, n - k) for kk in order(count(t, 1 - hf))])

    for t in range(2):
        relay(t, 0)

    def base_tile(i, _):
        for t in range(2):
            s = (i % 2) * 2 + t
            wait(w_copies(i, t))
            acc[t, i] = jnp.dot(x[...], wbuf[s, :chunks].reshape(width, tile), preferred_element_type=F32)

            @pl.when(i + 2 < tiles)
            def _():
                start(w_copies(i + 2, t))

            @pl.when(i + 2 >= tiles)
            def _():
                start(d_copies(i + 2 - tiles, t))
        return 0

    early = tiles // 8
    lax.fori_loop(0, early, base_tile, 0)
    for t in range(2):
        relay(t, 1)
    lax.fori_loop(early, tiles, base_tile, 0)
    for t, hf in downs:
        for k in range(1, count(t, hf)):
            stage1(t, hf, k).wait()
        for b in range(count(t, hf)):
            start([stage2(t, hf, k, b) for k in order(nz)])

    for t in range(2):
        for k in range(1, nq):
            packet(t, k).wait()
    for t, hf in both:
        for k in range(1, count(t, 1 - hf)):
            for b in range(count(t, hf)):
                stage2(t, hf, k, b).wait()

    def back(t, k, d):
        return pltpu.make_async_remote_copy(snd.at[t * nq + k], rec.at[t, mine[t]], d_s.at[t, k], d_r.at[t, mine[t]],
                                            device_id=member(t, d), device_id_type=mesh_id)

    def delta_step(k):
        aims = [target(t, k) for t in range(2)]
        for t in range(2):
            spread_low(rpk[t, aims[t]], spread.at[t], tokens)
            for hf in range(2):
                out_part = jnp.dot(spread[t], (b0, b1)[hf][t].reshape(rows, widths[hf]), preferred_element_type=F32)
                snd[t * nq + k, :, spans[hf]] = (SCALE * out_part).astype(BF)
        for t in range(2):
            @pl.when(k == nq - 1)
            def _():
                rec[t, mine[t]] = snd[t * nq + k]

            @pl.when(k < nq - 1)
            def _():
                back(t, k, aims[t]).start()

    def final(k):
        q = slab_at(k)
        for t in range(2):
            @pl.when(q != mine[t])
            def _():
                pltpu.make_async_remote_copy(snd.at[t * nq + k], rec.at[t, q], d_s.at[t, k], d_r.at[t, q],
                                             device_id=member(t, q), device_id_type=mesh_id).wait_recv()

        def gated(hf):
            cols = pl.ds(hf * tile, tile)
            g = acc[0, 2 * q + hf] + rec[0, q, :, cols].astype(F32)
            u = acc[1, 2 * q + hf] + rec[1, q, :, cols].astype(F32)
            rec[0, q, :, cols] = (g * jax.nn.sigmoid(g) * u).astype(BF)

        for hf in range(2):
            n = 2 * k + hf
            wait(d_copies(n, 0))
            wait(d_copies(n, 1))
            if hf == 0:
                gated(0)
            h = rec[0, q, :, pl.ds(hf * tile, tile)]
            turned = h.T
            for j in range(rows // tile):
                span = pl.ds(j * tile, tile)
                adn[span] += jnp.dot(wbuf[2 * hf, j], turned, preferred_element_type=F32)
            for j in range(chunks):
                span = pl.ds(j * tile, tile)
                y[:, span] += jnp.dot(h, wbuf[2 * hf + 1, j], preferred_element_type=F32)
            if hf == 0:
                gated(1)

            @pl.when(n + 2 < tiles)
            def _():
                for t in range(2):
                    start(d_copies(n + 2, t))

    y[...] = jnp.zeros_like(y)
    adn[...] = jnp.zeros_like(adn)
    lag = nq

    def middle(k, _):
        @pl.when(k < nq)
        def _():
            delta_step(k)

        @pl.when(k >= lag)
        def _():
            final(k - lag)
        return 0

    lax.fori_loop(0, nq + lag, middle, 0)

    low[0] = jnp.zeros_like(low[0])

    def down_block(i, _):
        adapter = (iota((ROWS, tokens), 0) + i * ROWS) >> 3
        kept = jnp.where(adapter == ids[...], adn[pl.ds(pl.multiple_of(i * ROWS, ROWS), ROWS)], 0.0).astype(BF)
        low[0] += jnp.dot(select_rows(8), kept, preferred_element_type=F32)
        return 0

    lax.fori_loop(0, nblk, down_block, 0)
    for t in (2, 3):
        send_packet(t, low[0])

    def sent(k, _):
        for t in range(2):
            d = target(t, k)

            @pl.when(k < nq - 1)
            def _():
                back(t, k, d).wait_send()
        return 0

    lax.fori_loop(0, nq, sent, 0)
    for t, hf in downs:
        for k in range(1, nz):
            for b in range(count(t, hf)):
                stage2(t, hf, k, b).wait()
        for k in range(1, nq):
            packet(t, k).wait()

    def down_back(t, k, q, d):
        w = pl.ds(0, w2 if t == 2 else w3)
        return pltpu.make_async_remote_copy(snd.at[(t - 2) * nq + k, :, w], rec.at[t - 2, q, :, w], d_s.at[t, k], d_r.at[t, q],
                                            device_id=member(t, d), device_id_type=mesh_id)

    def down_step(k, _):
        aims = [target(t, k) for t in (2, 3)]
        parts = [pl.ds(0, w2), pl.ds(0, w3)]
        for i in range(2):
            spread_low(rpk[i + 2, aims[i]], spread.at[i], tokens)
            delta = jnp.dot(spread[i], (b2, b3)[i][...].reshape(rows, (w2, w3)[i]), preferred_element_type=F32)
            snd[i * nq + k, :, parts[i]] = (SCALE * delta).astype(BF)
        for i in range(2):
            @pl.when(k == nq - 1)
            def _():
                rec[i, mine[i + 2], :, parts[i]] = snd[i * nq + k, :, parts[i]]

            @pl.when(k < nq - 1)
            def _():
                down_back(i + 2, k, mine[i + 2], aims[i]).start()
        return 0

    lax.fori_loop(0, nq, down_step, 0)

    def out_copy(t, q):
        w = w2 if t == 2 else w3
        cols = pl.ds(pl.multiple_of(q * w2 if t == 2 else nq * w2 + q * w3, 128), w)
        return pltpu.make_async_copy(rec.at[t - 2, q, :, pl.ds(0, w)], out.at[:, cols], o_sem.at[t - 2, q])

    def finish(k, _):
        q = slab_at(k)
        for t in (2, 3):
            @pl.when(q != mine[t])
            def _():
                down_back(t, k, q, q).wait_recv()
            w = w2 if t == 2 else w3
            cols = pl.ds(pl.multiple_of(q * w2 if t == 2 else nq * w2 + q * w3, 128), w)
            part = pl.ds(0, w)
            rec[t - 2, q, :, part] = (x[:, cols].astype(F32) + (y[:, cols] + rec[t - 2, q, :, part].astype(F32))).astype(BF)
            out_copy(t, q).start()
        return 0

    lax.fori_loop(0, nq, finish, 0)

    def down_sent(k, _):
        for t in (2, 3):
            d = target(t, k)

            @pl.when(k < nq - 1)
            def _():
                down_back(t, k, mine[t], d).wait_send()

            out_copy(t, k).wait()
        return 0

    lax.fori_loop(0, nq, down_sent, 0)


def layer_call(dims, x, ids, ag, au, wg, wu, bg, bu, ad, wd, bd):
    nx, ny, nz = dims
    nq = 2 * nx
    tokens, width = x.shape
    rows, hidden = ag.shape[0], wg.shape[1]
    slab = hidden // nq
    tile = slab // 2
    cut = max(128, slab // 4)
    w2 = width // (3 * nq) * 2
    w3 = width // (3 * nq)
    tiles = hidden // tile
    dma = pltpu.SemaphoreType.DMA
    vm = pl.BlockSpec(memory_space=pltpu.VMEM)
    anym = pl.BlockSpec(memory_space=pl.ANY)
    n1 = max(nx, ny, nz)
    nch = max(width, rows) // tile
    wide = width // slab
    return pl.pallas_call(
        functools.partial(layer_kernel, dims),
        out_shape=jax.ShapeDtypeStruct((tokens, width), BF),
        in_specs=[vm] * 2 + [anym] * 9,
        out_specs=anym,
        scratch_shapes=[
            pltpu.VMEM((4, nch, tile, tile), BF),
            pltpu.VMEM((2, tiles, tokens, tile), F32),
            pltpu.VMEM((2, nz, nx, nx * 32, cut), BF),
            pltpu.VMEM((2, nz, nx, nx * 32, slab - cut), BF),
            pltpu.VMEM((nz, nx, nx * 32, w2), BF),
            pltpu.VMEM((nz, nx, nx * 32, w3), BF),
            pltpu.VMEM((max(2 * nq, 5 * wide), tokens, slab), BF),
            pltpu.VMEM((2, nq, tokens, slab), BF),
            pltpu.VMEM((2, tokens, rows), BF),
            pltpu.VMEM((2, 16, tokens), F32),
            pltpu.VMEM((rows, tokens), F32),
            pltpu.VMEM((tokens, width), F32),
            pltpu.VMEM((4, 16, tokens), BF),
            pltpu.VMEM((4, nq, 16, tokens), BF),
            dma((4, nch)), dma((4, wide)),
            dma((6, nq)), dma((6, nq)), dma((6, n1)), dma((6, n1)), dma((6, n1, n1)), dma((6, n1, n1)),
            dma((6,)), dma((4, nq)), dma((4, nq)), dma((4, nq)), dma((4, nq)), dma((2, nq)),
        ],
        compiler_params=pltpu.CompilerParams(collective_id=0, has_side_effects=True, vmem_limit_bytes=67_000_000),
        cost_estimate=pl.CostEstimate(flops=6 * tokens * width * hidden, bytes_accessed=6 * width * hidden, transcendentals=tokens * hidden),
        name='layer',
    )(x, ids, ag, au, wg, wu, bg, bu, ad, wd, bd)


def solution(mesh, dims=(4, 4, 4)):
    row_spec = P(('rep', 'data'), None)
    tok_spec = P(('rep', 'data'))
    two = P(None, None)
    three = P(None, None, None)
    owned = P('data', None, None)

    def device_fn(x, ids, wg, wu, wd, ag, bg, au, bu, ad, bd):
        own, r = bg.shape[:2]
        adapters = ag.shape[0]
        flat = lambda a: jnp.transpose(a, (0, 2, 1)).reshape(adapters * r, a.shape[1])
        rows = lambda a: a.reshape(own * r, a.shape[2])
        return layer_call(dims, x, ids.reshape(1, -1), flat(ag), flat(au), wg, wu, rows(bg), rows(bu), flat(ad), wd, rows(bd))

    return jax.shard_map(device_fn, mesh=mesh, in_specs=(row_spec, tok_spec, two, two, two, three, owned, three, owned, three, owned), out_specs=row_spec, check_vma=False)
```
